32 devices in a mesh: dp: 2 (over x), tp: 4 (over z), cp: 4 (over y, core).
Axes of the slice: x: 2, y: 2, z: 4, core: 2. Of those that a mesh axis runs over, the one named last changes fastest.
Arguments:
- x: bfloat16 [8192, 3584], P(('dp', 'cp')), parts along dimension 0
- doc_ids: int32 [8192], P(('dp', 'cp')), parts along dimension 0
- w_query: bfloat16 [3584, 3584], P(None, 'tp')
- w_key: bfloat16 [3584, 512], P(None, 'tp')
- w_value: bfloat16 [3584, 512], P(None, 'tp')
- w_out: bfloat16 [3584, 3584], P('tp')
Outputs:
- output: bfloat16 [8192, 3584], P(('dp', 'cp')), parts along dimension 0
There are 2 independent parts. The reference program is written for one: setup_inputs(seed, part) draws one part's arguments, and reference() takes and returns one part's arrays. A program takes and returns all parts, laid end to end along the dimension named above; an argument that names none is the same for every part.
All inputs are finite; a program needn't handle non-finite values.
Results may differ from the reference program's by a relative error of at most 0.00734913.
Values are sent between devices in bfloat16 or wider.
A program may use at most 1 GiB of HBM per device.

```python
import jax
import jax.numpy as jnp
from jax import lax

SEQ_LEN = 4096
BLOCK_LEN = 256
DOC_BREAKS = 16
D = 3584
HEADS = 28
KV_HEADS = 4
HEAD = 128


def setup_inputs(seed: int = 0, part: int = 0) -> dict:
    shared_keys = jax.random.split(jax.random.key(seed), 4)
    part_keys = jax.random.split(jax.random.fold_in(jax.random.key(seed + 1), part), 4)
    x = jax.random.normal(part_keys[0], (SEQ_LEN, D), jnp.float32).astype(jnp.bfloat16)
    span_len = jax.random.randint(part_keys[1], (), SEQ_LEN // 3, 2 * SEQ_LEN // 3 + 1)
    span_start = jax.random.randint(part_keys[2], (), 0, SEQ_LEN - span_len + 1)
    breaks = jax.random.randint(part_keys[3], (DOC_BREAKS,), 1, SEQ_LEN)
    inside = (breaks > span_start) & (breaks < span_start + span_len)
    start_flags = jnp.zeros((SEQ_LEN,), jnp.int32).at[breaks].add(jnp.where(inside, 0, 1))
    doc_ids = jnp.cumsum(start_flags).astype(jnp.int32)
    w_query = (jax.random.normal(shared_keys[0], (D, HEADS * HEAD), jnp.float32) * (1.5 / D ** 0.5)).astype(jnp.bfloat16)
    w_key = (jax.random.normal(shared_keys[1], (D, KV_HEADS * HEAD), jnp.float32) * (1.5 / D ** 0.5)).astype(jnp.bfloat16)
    w_value = (jax.random.normal(shared_keys[2], (D, KV_HEADS * HEAD), jnp.float32) / D ** 0.5).astype(jnp.bfloat16)
    w_out = (jax.random.normal(shared_keys[3], (HEADS * HEAD, D), jnp.float32) * (2.0 / (HEADS * HEAD) ** 0.5)).astype(jnp.bfloat16)
    return {'x': x, 'doc_ids': doc_ids, 'w_query': w_query, 'w_key': w_key, 'w_value': w_value, 'w_out': w_out}


def block_update(soft_state, q_blk, k_blk, v_blk, allowed):
    run_max, run_sum, out_acc = soft_state
    scores = jnp.einsum('qhgd,khd->qhgk', q_blk.astype(jnp.float32), k_blk.astype(jnp.float32)) * (HEAD ** -0.5)
    scores = jnp.where(allowed[:, None, None, :], scores, -jnp.inf)
    new_max = jnp.maximum(run_max, jnp.max(scores, axis=-1))
    safe_max = jnp.where(new_max == -jnp.inf, 0.0, new_max)
    prob_vals = jnp.exp(scores - safe_max[..., None])
    rescale = jnp.exp(run_max - safe_max)
    run_sum = run_sum * rescale + jnp.sum(prob_vals, axis=-1)
    out_acc = out_acc * rescale[..., None] + jnp.einsum('qhgk,khd->qhgd', prob_vals, v_blk.astype(jnp.float32))
    return new_max, run_sum, out_acc


def reference(x, doc_ids, w_query, w_key, w_value, w_out):
    q_per_kv = HEADS // KV_HEADS
    n_blocks = SEQ_LEN // BLOCK_LEN
    q_all = jnp.dot(x, w_query, preferred_element_type=jnp.float32).astype(jnp.bfloat16).reshape(n_blocks, BLOCK_LEN, KV_HEADS, q_per_kv, HEAD)
    k_all = jnp.dot(x, w_key, preferred_element_type=jnp.float32).astype(jnp.bfloat16).reshape(n_blocks, BLOCK_LEN, KV_HEADS, HEAD)
    v_all = jnp.dot(x, w_value, preferred_element_type=jnp.float32).astype(jnp.bfloat16).reshape(n_blocks, BLOCK_LEN, KV_HEADS, HEAD)
    seg_blocks = doc_ids.reshape(n_blocks, BLOCK_LEN)
    pos_blocks = jnp.arange(SEQ_LEN).reshape(n_blocks, BLOCK_LEN)

    def query_block(q_inputs):
        q_blk, seg_q, pos_q = q_inputs

        def key_step(soft_state, k_inputs):
            k_blk, v_blk, seg_k, pos_k = k_inputs
            active = (pos_k[0] <= pos_q[BLOCK_LEN - 1]) & (seg_k[BLOCK_LEN - 1] >= seg_q[0])
            allowed = (seg_q[:, None] == seg_k[None, :]) & (pos_q[:, None] >= pos_k[None, :])
            new_state = lax.cond(active, lambda same_state: block_update(same_state, q_blk, k_blk, v_blk, allowed), lambda same_state: same_state, soft_state)
            return new_state, None

        init_state = (jnp.full((BLOCK_LEN, KV_HEADS, q_per_kv), -jnp.inf, jnp.float32), jnp.zeros((BLOCK_LEN, KV_HEADS, q_per_kv), jnp.float32), jnp.zeros((BLOCK_LEN, KV_HEADS, q_per_kv, HEAD), jnp.float32))
        final_state = lax.scan(key_step, init_state, (k_all, v_all, seg_blocks, pos_blocks))[0]
        run_sum = final_state[1]
        out_acc = final_state[2]
        return (out_acc / run_sum[..., None]).astype(jnp.bfloat16).reshape(BLOCK_LEN, HEADS * HEAD)

    heads_out = lax.map(query_block, (q_all, seg_blocks, pos_blocks)).reshape(SEQ_LEN, HEADS * HEAD)
    return jnp.dot(heads_out, w_out, preferred_element_type=jnp.float32).astype(jnp.bfloat16)
```

```python
import functools

import jax
import jax.numpy as jnp
from jax import lax
from jax.experimental import pallas as pl
from jax.experimental.pallas import tpu as pltpu
from jax.sharding import PartitionSpec as P

HEAD_DIM = 128
MESH = pl.DeviceIdType.MESH
LOG2_SCALE = (HEAD_DIM ** -0.5) * 1.4426950408889634
F32 = jnp.float32
BF16 = jnp.bfloat16

Q_BLK = 256
LOC_BLK = 512
O_ROWS = 128


def coords():
    return lax.axis_index('dp'), lax.axis_index('tp'), lax.axis_index('cp')


def greet(dp, tp, cp, mid):
    bar = pltpu.get_barrier_semaphore()

    def hello(dev):
        pl.semaphore_signal(bar, inc=1, device_id=dev, device_id_type=MESH)

    hello((1 - dp, tp, cp))
    hello((dp, tp, lax.rem(cp + 2, 4)))
    hello((dp, tp, cp + 1 - 2 * lax.rem(cp, 2)))
    pl.when(tp > 0)(lambda: hello((dp, tp - 1, cp)))
    pl.when(tp < 3)(lambda: hello((dp, tp + 1, cp)))
    pl.semaphore_wait(bar, 4 + mid)


def peer_shard(tp, k):
    if k == 1:
        return tp + 1 - 2 * lax.rem(tp, 2)
    if k == 2:
        return lax.rem(tp + 2, 4)
    return 3 - tp


def attend_kernel(x_hbm, seg_col, seg_row, wq_hbm, wk_hbm, wv_hbm, wo_hbm, o_ref, wz_hbm,
                  x_v, wq_v, wkv_v, q_v, kv_v, seg_v, bias_v, m_v, l_v, acc_v,
                  load_sem, kv_send, kv_recv, seg_send, seg_recv, z_send, z_recv):
    dp, tp, cp = coords()
    mid = lax.rem((tp + 1) // 2, 2)
    core = lax.rem(cp, 2)
    chunk = x_v.shape[0]
    heads = q_v.shape[1] // HEAD_DIM
    n_rows = wo_hbm.shape[0] // 8
    n_blk = chunk // Q_BLK

    loads = []
    for i in range(n_blk):
        rows = slice(i * Q_BLK, (i + 1) * Q_BLK)
        loads.append(pltpu.make_async_copy(x_hbm.at[rows], x_v.at[rows], load_sem.at[i]))
    k_load = pltpu.make_async_copy(wk_hbm, wkv_v.at[:, 0:HEAD_DIM], load_sem.at[n_blk])
    v_load = pltpu.make_async_copy(wv_hbm, wkv_v.at[:, HEAD_DIM:2 * HEAD_DIM], load_sem.at[n_blk + 1])
    q_load = pltpu.make_async_copy(wq_hbm, wq_v, load_sem.at[n_blk + 2])
    k_load.start()
    v_load.start()
    for load in loads:
        load.start()
    q_load.start()

    greet(dp, tp, cp, mid)

    mine = pl.ds(pl.multiple_of((dp * 4 + cp) * n_rows, 16), n_rows)

    def z_copy(slot, src, shard, to):
        return pltpu.make_async_remote_copy(src, wz_hbm.at[shard], z_send.at[slot], z_recv.at[shard],
                                            device_id=(dp, to, cp), device_id_type=MESH)

    z_up = z_copy(0, wo_hbm.at[mine], tp, tp + 1)
    z_down = z_copy(4, wo_hbm.at[mine], tp, tp - 1)
    pl.when(tp < 3)(z_up.start)
    pl.when(tp > 0)(z_down.start)

    def z_next(k):
        shard = peer_shard(tp, k)
        to = tp + 1 - 2 * (shard // (tp + 1) > 0).astype(jnp.int32)
        return z_copy(k, wz_hbm.at[shard], shard, to)

    def z_forward(k):
        z_next(k).wait_recv()

        @pl.when(mid == 1)
        def _():
            z_next(k).start()

    own = pl.ds(pl.multiple_of(cp * chunk, chunk), chunk)
    k_load.wait()
    v_load.wait()
    for i in range(n_blk):
        loads[i].wait()
        rows = slice(i * Q_BLK, (i + 1) * Q_BLK)
        kv_v[pl.ds(pl.multiple_of(cp * chunk + i * Q_BLK, Q_BLK), Q_BLK), :] = jnp.dot(
            x_v[rows, :], wkv_v[...], preferred_element_type=F32).astype(BF16)
    seg_load = pltpu.make_async_copy(seg_row, seg_v.at[:, own], load_sem.at[n_blk + 3])
    seg_load.start()
    seg_load.wait()

    def kv_copies(slot, block, to):
        rows = pl.ds(pl.multiple_of(block * chunk, chunk), chunk)
        dev = (dp, tp, to)
        return (pltpu.make_async_remote_copy(kv_v.at[rows], kv_v.at[rows], kv_send.at[slot], kv_recv.at[slot],
                                             device_id=dev, device_id_type=MESH),
                pltpu.make_async_remote_copy(seg_v.at[:, rows], seg_v.at[:, rows], seg_send.at[slot], seg_recv.at[slot],
                                             device_id=dev, device_id_type=MESH))

    def over(copies, what):
        for copy in copies:
            getattr(copy, what)()

    other_core = cp + 1 - 2 * core

    q_load.wait()

    def project(i):
        rows = pl.ds(pl.multiple_of(i * Q_BLK, Q_BLK), Q_BLK)
        q_v[rows, :] = jnp.dot(x_v[rows, :], wq_v[...], preferred_element_type=F32).astype(BF16)

    project(0)
    pl.when(cp < 2)(lambda: over(kv_copies(0, cp, lax.rem(cp + 2, 4)), 'start'))
    pl.when(core == 0)(lambda: over(kv_copies(1, cp, other_core), 'start'))

    @pl.loop(1, n_blk)
    def _(i):
        project(i)

    def step(i, key0, n_keys, first, local):
        rows = pl.ds(pl.multiple_of(i * Q_BLK, Q_BLK), Q_BLK)
        keys = pl.ds(pl.multiple_of(key0, n_keys), n_keys)
        groups = n_keys // HEAD_DIM
        q_seg = seg_col[rows, :]
        for g in range(groups):
            cols = pl.ds(pl.multiple_of(key0 + g * HEAD_DIM, HEAD_DIM), HEAD_DIM)
            ok = q_seg == seg_v[0:1, cols]
            if local:
                q_pos = cp * chunk + i * Q_BLK + lax.broadcasted_iota(jnp.int32, (Q_BLK, HEAD_DIM), 0)
                k_pos = key0 + g * HEAD_DIM + lax.broadcasted_iota(jnp.int32, (Q_BLK, HEAD_DIM), 1)
                ok = ok & (q_pos >= k_pos)
            bias_v[:, g * HEAD_DIM:(g + 1) * HEAD_DIM] = jnp.where(ok, 0.0, -jnp.inf)
        k_blk = kv_v[keys, 0:HEAD_DIM]
        v_blk = kv_v[keys, HEAD_DIM:2 * HEAD_DIM]
        for h in range(heads):
            cols = slice(h * HEAD_DIM, (h + 1) * HEAD_DIM)
            s = lax.dot_general(q_v[rows, cols], k_blk, (((1,), (1,)), ((), ())), preferred_element_type=F32)
            s = [s[:, g * HEAD_DIM:(g + 1) * HEAD_DIM] + bias_v[:, g * HEAD_DIM:(g + 1) * HEAD_DIM] for g in range(groups)]
            top = functools.reduce(jnp.maximum, s)
            top = jnp.max(top, axis=1, keepdims=True)
            if first:
                m_new = jnp.broadcast_to(top, (Q_BLK, HEAD_DIM))
            else:
                m_old = m_v[rows, cols]
                m_new = jnp.maximum(m_old, top)
                fade = jnp.exp2((m_old - m_new) * LOG2_SCALE)
            p = [jnp.exp2((part - m_new) * LOG2_SCALE) for part in s]
            total = functools.reduce(jnp.add, p)
            probs = jnp.concatenate([part.astype(BF16) for part in p], axis=1)
            pv = jnp.dot(probs, v_blk, preferred_element_type=F32)
            m_v[rows, cols] = m_new
            if first:
                l_v[rows, cols] = total
                acc_v[rows, cols] = pv
            else:
                l_v[rows, cols] = l_v[rows, cols] * fade + total
                acc_v[rows, cols] = acc_v[rows, cols] * fade + pv

    per_loc = LOC_BLK // Q_BLK

    def local_pass(i):
        last = i // per_loc
        step(i, cp * chunk + last * LOC_BLK, LOC_BLK, True, True)

        @pl.loop(0, last)
        def _(j):
            step(i, cp * chunk + j * LOC_BLK, LOC_BLK, False, False)

    @pl.loop(0, n_blk)
    def _(i):
        local_pass(i)

    z_forward(1)
    z_forward(3)

    @pl.when(cp >= 2)
    def _():
        over(kv_copies(0, cp - 2, cp), 'wait_recv')
        over(kv_copies(2, cp - 2, other_core), 'start')
        over(kv_copies(2, other_core - 2, cp), 'wait_recv')

    @pl.when(core == 1)
    def _():
        over(kv_copies(1, other_core, cp), 'wait_recv')

    def finish(i):
        rows = pl.ds(pl.multiple_of(i * Q_BLK, Q_BLK), Q_BLK)
        for h in range(heads):
            cols = slice(h * HEAD_DIM, (h + 1) * HEAD_DIM)
            total = jnp.sum(l_v[rows, cols], axis=1, keepdims=True)
            o_ref[rows, cols] = (acc_v[rows, cols] / total).astype(BF16)

    @pl.loop(0, n_blk)
    def _(i):
        @pl.loop(0, cp)
        def _(j):
            step(i, j * chunk, chunk, False, False)

        finish(i)

        @pl.when(i == 1)
        def _():
            z_forward(2)

    pl.when(cp < 2)(lambda: over(kv_copies(0, cp, lax.rem(cp + 2, 4)), 'wait_send'))
    pl.when(core == 0)(lambda: over(kv_copies(1, cp, other_core), 'wait_send'))
    pl.when(cp >= 2)(lambda: over(kv_copies(2, cp - 2, other_core), 'wait_send'))
    pl.when(tp < 3)(z_up.wait_send)
    pl.when(tp > 0)(z_down.wait_send)

    @pl.when(mid == 1)
    def _():
        for k in (1, 2, 3):
            z_next(k).wait_send()


def output_kernel(o_hbm, wo_hbm, wz_hbm, y_hbm, w_v, o_v, acc_v, y_v,
                  load_sem, own_sem, w_send, w_recv, o_send, o_recv, y_sem):
    dp, tp, cp = coords()
    mid = lax.rem((tp + 1) // 2, 2)
    chunk, width = o_hbm.shape
    n_cols = wo_hbm.shape[1]
    n_rows = width // 8
    half = n_cols // 2
    n_pc = chunk // O_ROWS
    cp_y = lax.rem(cp + 2, 4)
    cp_c = cp + 1 - 2 * lax.rem(cp, 2)
    dev_x, dev_y, dev_c = (1 - dp, tp, cp), (dp, tp, cp_y), (dp, tp, cp_c)

    own_w = pltpu.make_async_copy(wo_hbm, w_v.at[0], load_sem.at[0])
    own_o = pltpu.make_async_copy(o_hbm, o_v.at[tp], load_sem.at[1])
    own_w.start()
    own_o.start()

    greet(dp, tp, cp, mid)

    def piece(c):
        return pl.ds(pl.multiple_of(c * O_ROWS, O_ROWS), O_ROWS)

    def o_copy(slot, c, src, shard, to):
        return pltpu.make_async_remote_copy(src, o_v.at[shard, piece(c)], o_send.at[slot, c], o_recv.at[shard, c],
                                            device_id=(dp, to, cp), device_id_type=MESH)

    def o_up(c):
        return o_copy(0, c, o_hbm.at[piece(c)], tp, tp + 1)

    def o_down(c):
        return o_copy(4, c, o_hbm.at[piece(c)], tp, tp - 1)

    @pl.loop(0, n_pc)
    def _(c):
        pl.when(tp < 3)(lambda: o_up(c).start())
        pl.when(tp > 0)(lambda: o_down(c).start())

    def o_next(k, c):
        shard = peer_shard(tp, k)
        to = tp + 1 - 2 * (shard // (tp + 1) > 0).astype(jnp.int32)
        return o_copy(k, c, o_v.at[shard, piece(c)], shard, to)

    def o_forward(k, c):
        o_next(k, c).wait_recv()
        pl.when(mid == 1)(lambda: o_next(k, c).start())

    def rows_of(dp_i, cp_i):
        return pl.ds(pl.multiple_of((dp_i * 4 + cp_i) * n_rows, 16), n_rows)

    cols = {'a': pl.ds(0, half), 'b': pl.ds(half, half), 'ab': pl.ds(0, n_cols)}
    hops = [('x', 'own', 'a'), ('x', 'own', 'b'), ('x', 'y', 'b'), ('y', 'own', 'b'), ('y', 'own', 'a'), ('y', 'x', 'a'),
            ('c', 'own', 'ab'), ('c', 'x', 'a'), ('c', 'x', 'b'), ('c', 'd', 'b'), ('c', 'y', 'b'), ('c', 'y', 'a'), ('c', 'd', 'a')]

    def slice_rows(name, dp_i, cp_i):
        far = lax.rem(cp_i + 2, 4)
        return {'own': rows_of(dp_i, cp_i), 'x': rows_of(1 - dp_i, cp_i), 'y': rows_of(dp_i, far), 'd': rows_of(1 - dp_i, far)}[name]

    def w_copy(k, hop):
        route, name, part = hops[hop]
        rows, cut = slice_rows(name, dp, cp), cols[part]
        dst = w_v.at[k, rows, cut]
        src = wz_hbm.at[peer_shard(tp, k), :, cut] if name == 'own' else dst
        dev = {'x': dev_x, 'y': dev_y, 'c': dev_c}[route]
        return pltpu.make_async_remote_copy(src, dst, w_send.at[k - 1, hop], w_recv.at[k - 1, hop], device_id=dev, device_id_type=MESH)

    def w_arrival(k, hop):
        route, name, part = hops[hop]
        dp_i, cp_i = {'x': (1 - dp, cp), 'y': (dp, cp_y), 'c': (dp, cp_c)}[route]
        dst = w_v.at[k, slice_rows(name, dp_i, cp_i), cols[part]]
        dev = {'x': dev_x, 'y': dev_y, 'c': dev_c}[route]
        return pltpu.make_async_remote_copy(dst, dst, w_send.at[k - 1, hop], w_recv.at[k - 1, hop], device_id=dev, device_id_type=MESH)

    own_slices = [pltpu.make_async_copy(wz_hbm.at[peer_shard(tp, k)], w_v.at[k, rows_of(dp, cp)], own_sem.at[k - 1]) for k in (1, 2, 3)]
    for k in (1, 2, 3):
        w_copy(k, 0).start()
        w_copy(k, 3).start()
        w_copy(k, 6).start()
        own_slices[k - 1].start()
    for k in (1, 2, 3):
        w_copy(k, 1).start()
        w_copy(k, 4).start()

    n_tile = 512

    def multiply(k, c, store):
        shard = tp if k == 0 else peer_shard(tp, k)
        lhs = o_v[shard, piece(c), :]

        @pl.loop(0, n_cols // n_tile)
        def _(n):
            out = pl.ds(pl.multiple_of(n * n_tile, n_tile), n_tile)
            part = jnp.dot(lhs, w_v[k, :, out], preferred_element_type=F32)
            store(out, part)

    own_w.wait()
    own_o.wait()

    @pl.loop(0, n_pc)
    def _(c):
        def store(out, part):
            acc_v[piece(c), out] = part

        multiply(0, c, store)

    for k in (1, 2, 3):
        w_arrival(k, 0).wait_recv()
        w_copy(k, 5).start()
        w_copy(k, 7).start()
        w_arrival(k, 3).wait_recv()
        w_copy(k, 2).start()
        w_copy(k, 10).start()

    @pl.loop(0, n_pc)
    def _(c):
        o_forward(1, c)

        @pl.when(mid == 1)
        def _():
            o_forward(3, c)

    for k in (1, 2, 3):
        w_arrival(k, 1).wait_recv()
        w_copy(k, 8).start()
        w_arrival(k, 4).wait_recv()
        w_copy(k, 11).start()

    def w_finish(k):
        w_arrival(k, 2).wait_recv()
        w_copy(k, 9).start()
        w_arrival(k, 5).wait_recv()
        w_copy(k, 12).start()
        for hop in range(6, 13):
            w_arrival(k, hop).wait_recv()
        own_slices[k - 1].wait()

    w_finish(1)

    @pl.loop(0, n_pc)
    def _(c):
        def store(out, part):
            acc_v[piece(c), out] += part

        multiply(1, c, store)

    w_finish(2)

    @pl.loop(0, n_pc)
    def _(c):
        def store(out, part):
            acc_v[piece(c), out] += part

        o_forward(2, c)
        multiply(2, c, store)

    w_finish(3)

    def y_copy(slot, c):
        return pltpu.make_async_copy(y_v.at[slot], y_hbm.at[piece(c)], y_sem.at[slot])

    @pl.loop(0, n_pc)
    def _(c):
        slot = lax.rem(c, 2)
        pl.when(mid == 0)(lambda: o_next(3, c).wait_recv())
        pl.when(c >= 2)(lambda: y_copy(slot, c - 2).wait())

        def store(out, part):
            y_v[slot, :, out] = (acc_v[piece(c), out] + part).astype(BF16)

        multiply(3, c, store)
        y_copy(slot, c).start()

    for c in (n_pc - 2, n_pc - 1):
        y_copy(c % 2, c).wait()
    for k in (1, 2, 3):
        for hop in range(len(hops)):
            w_copy(k, hop).wait_send()

    @pl.loop(0, n_pc)
    def _(c):
        pl.when(tp < 3)(lambda: o_up(c).wait_send())
        pl.when(tp > 0)(lambda: o_down(c).wait_send())

        @pl.when(mid == 1)
        def _():
            for k in (1, 2, 3):
                o_next(k, c).wait_send()


def solution(mesh):
    any_spec = pl.BlockSpec(memory_space=pl.ANY)
    vmem_spec = pl.BlockSpec(memory_space=pltpu.VMEM)
    dma = pltpu.SemaphoreType.DMA

    def layer(x_loc, seg_loc, w_query, w_key, w_value, w_out):
        chunk, width = x_loc.shape
        q_cols = w_query.shape[1]
        n_rows = w_out.shape[0] // 8
        n_blk = chunk // Q_BLK
        seg_col = jnp.broadcast_to(seg_loc[:, None], (chunk, HEAD_DIM))
        seg_row = jnp.broadcast_to(seg_loc[None, :], (8, chunk))
        heads_out, w_slices = pl.pallas_call(
            attend_kernel,
            name='attend',
            out_shape=(jax.ShapeDtypeStruct((chunk, q_cols), BF16), jax.ShapeDtypeStruct((4, n_rows, w_out.shape[1]), BF16)),
            in_specs=[any_spec, vmem_spec, any_spec, any_spec, any_spec, any_spec, any_spec],
            out_specs=(vmem_spec, any_spec),
            scratch_shapes=[
                pltpu.VMEM((chunk, width), BF16),
                pltpu.VMEM((width, q_cols), BF16),
                pltpu.VMEM((width, 2 * HEAD_DIM), BF16),
                pltpu.VMEM((chunk, q_cols), BF16),
                pltpu.VMEM((4 * chunk, 2 * HEAD_DIM), BF16),
                pltpu.VMEM((8, 4 * chunk), jnp.int32),
                pltpu.VMEM((Q_BLK, chunk), F32),
                pltpu.VMEM((chunk, q_cols), F32),
                pltpu.VMEM((chunk, q_cols), F32),
                pltpu.VMEM((chunk, q_cols), F32),
                dma((n_blk + 4,)), dma((3,)), dma((3,)), dma((3,)), dma((3,)), dma((5,)), dma((4,)),
            ],
            compiler_params=pltpu.CompilerParams(collective_id=0, has_side_effects=True, vmem_limit_bytes=62 << 20),
        )(x_loc, seg_col, seg_row, w_query, w_key, w_value, w_out)
        n_pc = chunk // O_ROWS
        return pl.pallas_call(
            output_kernel,
            name='output',
            out_shape=jax.ShapeDtypeStruct((chunk, w_out.shape[1]), BF16),
            in_specs=[any_spec, any_spec, any_spec],
            out_specs=any_spec,
            scratch_shapes=[
                pltpu.VMEM((4,) + w_out.shape, BF16),
                pltpu.VMEM((4, chunk, q_cols), BF16),
                pltpu.VMEM((chunk, w_out.shape[1]), F32),
                pltpu.VMEM((2, O_ROWS, w_out.shape[1]), BF16),
                dma((2,)), dma((3,)), dma((3, 13)), dma((3, 13)), dma((5, n_pc)), dma((4, n_pc)), dma((2,)),
            ],
            compiler_params=pltpu.CompilerParams(collective_id=1, has_side_effects=True, vmem_limit_bytes=62 << 20),
        )(heads_out, w_out, w_slices)

    return jax.shard_map(layer, mesh=mesh, in_specs=(P(('dp', 'cp'), None), P(('dp', 'cp')), P(None, 'tp'), P(None, 'tp'), P(None, 'tp'), P('tp', None)), out_specs=P(('dp', 'cp'), None), check_vma=False)
```

```python
import functools

import jax
import jax.numpy as jnp
from jax import lax
from jax.experimental import pallas as pl
from jax.experimental.pallas import tpu as pltpu
from jax.sharding import PartitionSpec as P

HEAD_DIM = 128
MESH = pl.DeviceIdType.MESH
LOG2_SCALE = (HEAD_DIM ** -0.5) * 1.4426950408889634
F32 = jnp.float32
BF16 = jnp.bfloat16

Q_BLK = 256
LOC_BLK = 512
O_ROWS = 128


def coords():
    return lax.axis_index('dp'), lax.axis_index('tp'), lax.axis_index('cp')


def greet(dp, tp, cp, mid):
    bar = pltpu.get_barrier_semaphore()

    def hello(dev):
        pl.semaphore_signal(bar, inc=1, device_id=dev, device_id_type=MESH)

    hello((1 - dp, tp, cp))
    hello((dp, tp, lax.rem(cp + 2, 4)))
    hello((dp, tp, cp + 1 - 2 * lax.rem(cp, 2)))
    pl.when(tp > 0)(lambda: hello((dp, tp - 1, cp)))
    pl.when(tp < 3)(lambda: hello((dp, tp + 1, cp)))
    pl.semaphore_wait(bar, 4 + mid)


def peer_shard(tp, k):
    if k == 1:
        return tp + 1 - 2 * lax.rem(tp, 2)
    if k == 2:
        return lax.rem(tp + 2, 4)
    return 3 - tp


def layer_kernel(x_hbm, seg_hbm, wq_hbm, wk_hbm, wv_hbm, wo_hbm, y_hbm,
                 w_v, o_v, kv_v, seg_v,
                 load_sem, kv_send, kv_recv, seg_send, seg_recv, z_send, z_recv, w_send, w_recv, o_send, o_recv, y_sem):
    dp, tp, cp = coords()
    mid = lax.rem((tp + 1) // 2, 2)
    core = lax.rem(cp, 2)
    chunk, d_model = x_hbm.shape
    q_cols = wq_hbm.shape[1]
    heads = q_cols // HEAD_DIM
    n_rows = wo_hbm.shape[0] // 8
    n_cols = wo_hbm.shape[1]
    half = n_cols // 2
    n_blk = chunk // Q_BLK
    n_pc = chunk // O_ROWS
    per_blk = Q_BLK // O_ROWS
    cp_y = lax.rem(cp + 2, 4)
    cp_c = cp + 1 - 2 * core
    dev_x, dev_y, dev_c = (1 - dp, tp, cp), (dp, tp, cp_y), (dp, tp, cp_c)

    def onward(shard):
        return tp + 1 - 2 * (shard // (tp + 1) > 0).astype(jnp.int32)

    def rows_of(dp_i, cp_i):
        return pl.ds(pl.multiple_of((dp_i * 4 + cp_i) * n_rows, 16), n_rows)

    def z_copy(slot, src, shard, to):
        return pltpu.make_async_remote_copy(src, w_v.at[shard, rows_of(dp, cp)], z_send.at[slot], z_recv.at[shard],
                                            device_id=(dp, to, cp), device_id_type=MESH)

    z_up = z_copy(0, wo_hbm.at[rows_of(dp, cp)], tp, tp + 1)
    z_down = z_copy(4, wo_hbm.at[rows_of(dp, cp)], tp, tp - 1)

    def z_next(k):
        shard = peer_shard(tp, k)
        return z_copy(k, w_v.at[shard, rows_of(dp, cp)], shard, onward(shard))

    cuts = {'a': pl.ds(0, half), 'b': pl.ds(half, half), 'ab': pl.ds(0, n_cols)}
    hops = [('x', 'own', 'a'), ('x', 'own', 'b'), ('x', 'y', 'b'), ('y', 'own', 'b'), ('y', 'own', 'a'), ('y', 'x', 'a'),
            ('c', 'own', 'ab'), ('c', 'x', 'a'), ('c', 'x', 'b'), ('c', 'd', 'b'), ('c', 'y', 'b'), ('c', 'y', 'a'), ('c', 'd', 'a')]

    def slice_rows(name, dp_i, cp_i):
        far = lax.rem(cp_i + 2, 4)
        return {'own': rows_of(dp_i, cp_i), 'x': rows_of(1 - dp_i, cp_i), 'y': rows_of(dp_i, far), 'd': rows_of(1 - dp_i, far)}[name]

    def w_hop(k, hop, dp_i, cp_i):
        route, name, part = hops[hop]
        at = w_v.at[peer_shard(tp, k), slice_rows(name, dp_i, cp_i), cuts[part]]
        dev = {'x': dev_x, 'y': dev_y, 'c': dev_c}[route]
        return pltpu.make_async_remote_copy(at, at, w_send.at[k - 1, hop], w_recv.at[k - 1, hop], device_id=dev, device_id_type=MESH)

    def w_copy(k, hop):
        return w_hop(k, hop, dp, cp)

    def w_arrival(k, hop):
        dp_i, cp_i = {'x': (1 - dp, cp), 'y': (dp, cp_y), 'c': (dp, cp_c)}[hops[hop][0]]
        return w_hop(k, hop, dp_i, cp_i)

    def w_enter(k):
        z_next(k).wait_recv()
        pl.when(mid == 1)(lambda: z_next(k).start())
        for hop in (0, 3, 6, 1, 4):
            w_copy(k, hop).start()

    def piece(c):
        return pl.ds(pl.multiple_of(c * O_ROWS, O_ROWS), O_ROWS)

    def o_copy(slot, c, shard, to):
        at = o_v.at[shard, piece(c)]
        return pltpu.make_async_remote_copy(at, at, o_send.at[slot, c], o_recv.at[shard, c], device_id=(dp, to, cp), device_id_type=MESH)

    def o_up(c):
        return o_copy(0, c, tp, tp + 1)

    def o_down(c):
        return o_copy(4, c, tp, tp - 1)

    def o_leave(i):
        for j in range(per_blk):
            pl.when(tp < 3)(lambda: o_up(i * per_blk + j).start())
            pl.when(tp > 0)(lambda: o_down(i * per_blk + j).start())

    def o_next(k, c):
        shard = peer_shard(tp, k)
        return o_copy(k, c, shard, onward(shard))

    def o_forward(k, c):
        o_next(k, c).wait_recv()
        pl.when(mid == 1)(lambda: o_next(k, c).start())

    def kv_copies(slot, block, to):
        rows = pl.ds(pl.multiple_of(block * chunk, chunk), chunk)
        dev = (dp, tp, to)
        return (pltpu.make_async_remote_copy(kv_v.at[rows], kv_v.at[rows], kv_send.at[slot], kv_recv.at[slot],
                                             device_id=dev, device_id_type=MESH),
                pltpu.make_async_remote_copy(seg_v.at[:, rows], seg_v.at[:, rows], seg_send.at[slot], seg_recv.at[slot],
                                             device_id=dev, device_id_type=MESH))

    def over(copies, what):
        for copy in copies:
            getattr(copy, what)()

    own_w = pltpu.make_async_copy(wo_hbm, w_v.at[tp], load_sem.at[n_blk + 4])

    def attend(x_v, wq_v, wkv_v, q_v, col_v, bias_v, m_v, l_v, acc_v):
        loads = []
        for i in range(n_blk):
            rows = slice(i * Q_BLK, (i + 1) * Q_BLK)
            loads.append(pltpu.make_async_copy(x_hbm.at[rows], x_v.at[rows], load_sem.at[i]))
        k_load = pltpu.make_async_copy(wk_hbm, wkv_v.at[:, 0:HEAD_DIM], load_sem.at[n_blk])
        v_load = pltpu.make_async_copy(wv_hbm, wkv_v.at[:, HEAD_DIM:2 * HEAD_DIM], load_sem.at[n_blk + 1])
        q_load = pltpu.make_async_copy(wq_hbm, wq_v, load_sem.at[n_blk + 2])
        own = pl.ds(pl.multiple_of(cp * chunk, chunk), chunk)
        seg_load = pltpu.make_async_copy(seg_hbm, seg_v.at[:, own], load_sem.at[n_blk + 3])
        k_load.start()
        v_load.start()
        for load in loads:
            load.start()
        q_load.start()
        seg_load.start()
        own_w.start()

        greet(dp, tp, cp, mid)
        pl.when(tp < 3)(z_up.start)
        pl.when(tp > 0)(z_down.start)

        k_load.wait()
        v_load.wait()
        for i in range(n_blk):
            loads[i].wait()
            rows = slice(i * Q_BLK, (i + 1) * Q_BLK)
            kv_v[pl.ds(pl.multiple_of(cp * chunk + i * Q_BLK, Q_BLK), Q_BLK), :] = jnp.dot(
                x_v[rows, :], wkv_v[...], preferred_element_type=F32).astype(BF16)

        q_load.wait()

        def project(i):
            rows = pl.ds(pl.multiple_of(i * Q_BLK, Q_BLK), Q_BLK)
            q_v[rows, :] = jnp.dot(x_v[rows, :], wq_v[...], preferred_element_type=F32).astype(BF16)

        project(0)
        seg_load.wait()
        pl.when(cp < 2)(lambda: over(kv_copies(0, cp, cp_y), 'start'))
        pl.when(core == 0)(lambda: over(kv_copies(1, cp, cp_c), 'start'))

        @pl.loop(1, n_blk)
        def _(i):
            project(i)

        @pl.loop(0, chunk // HEAD_DIM)
        def _(i):
            ids = seg_v[0:1, pl.ds(pl.multiple_of(cp * chunk + i * HEAD_DIM, HEAD_DIM), HEAD_DIM)]
            rows = pl.ds(pl.multiple_of(i * HEAD_DIM, HEAD_DIM), HEAD_DIM)
            col_v[rows, :] = jnp.transpose(jnp.broadcast_to(ids, (HEAD_DIM, HEAD_DIM)))

        w_enter(1)
        pl.when(mid == 1)(lambda: w_enter(3))

        @pl.when(cp >= 2)
        def _():
            over(kv_copies(0, cp - 2, cp), 'wait_recv')
            over(kv_copies(2, cp - 2, cp_c), 'start')
            over(kv_copies(2, cp_c - 2, cp), 'wait_recv')

        @pl.when(core == 1)
        def _():
            over(kv_copies(1, cp_c, cp), 'wait_recv')

        def step(i, key0, n_keys, first):
            rows = pl.ds(pl.multiple_of(i * Q_BLK, Q_BLK), Q_BLK)
            keys = pl.ds(pl.multiple_of(key0, n_keys), n_keys)
            groups = n_keys // HEAD_DIM
            q_seg = col_v[rows, :]
            for g in range(groups):
                cols = pl.ds(pl.multiple_of(key0 + g * HEAD_DIM, HEAD_DIM), HEAD_DIM)
                ok = q_seg == seg_v[0:1, cols]
                if first:
                    q_pos = cp * chunk + i * Q_BLK + lax.broadcasted_iota(jnp.int32, (Q_BLK, HEAD_DIM), 0)
                    k_pos = key0 + g * HEAD_DIM + lax.broadcasted_iota(jnp.int32, (Q_BLK, HEAD_DIM), 1)
                    ok = ok & (q_pos >= k_pos)
                bias_v[:, g * HEAD_DIM:(g + 1) * HEAD_DIM] = jnp.where(ok, 0.0, -jnp.inf)
            k_blk = kv_v[keys, 0:HEAD_DIM]
            v_blk = kv_v[keys, HEAD_DIM:2 * HEAD_DIM]
            for h in range(heads):
                cols = slice(h * HEAD_DIM, (h + 1) * HEAD_DIM)
                s = lax.dot_general(q_v[rows, cols], k_blk, (((1,), (1,)), ((), ())), preferred_element_type=F32)
                s = [s[:, g * HEAD_DIM:(g + 1) * HEAD_DIM] + bias_v[:, g * HEAD_DIM:(g + 1) * HEAD_DIM] for g in range(groups)]
                top = jnp.max(functools.reduce(jnp.maximum, s), axis=1, keepdims=True)
                if first:
                    m_new = jnp.broadcast_to(top, (Q_BLK, HEAD_DIM))
                else:
                    m_old = m_v[:, cols]
                    m_new = jnp.maximum(m_old, top)
                    fade = jnp.exp2((m_old - m_new) * LOG2_SCALE)
                p = [jnp.exp2((part - m_new) * LOG2_SCALE) for part in s]
                total = functools.reduce(jnp.add, p)
                probs = jnp.concatenate([part.astype(BF16) for part in p], axis=1)
                pv = jnp.dot(probs, v_blk, preferred_element_type=F32)
                m_v[:, cols] = m_new
                if first:
                    l_v[:, cols] = total
                    acc_v[:, cols] = pv
                else:
                    l_v[:, cols] = l_v[:, cols] * fade + total
                    acc_v[:, cols] = acc_v[:, cols] * fade + pv

        per_loc = LOC_BLK // Q_BLK

        @pl.loop(0, n_blk)
        def _(i):
            last = i // per_loc
            step(i, cp * chunk + last * LOC_BLK, LOC_BLK, True)
            pl.when(i > 0)(lambda: o_leave(i - 1))

            @pl.loop(0, last)
            def _(j):
                step(i, cp * chunk + j * LOC_BLK, LOC_BLK, False)

            @pl.loop(0, cp)
            def _(j):
                step(i, j * chunk, chunk, False)

            rows = pl.ds(pl.multiple_of(i * Q_BLK, Q_BLK), Q_BLK)
            for h in range(heads):
                cols = slice(h * HEAD_DIM, (h + 1) * HEAD_DIM)
                total = jnp.sum(l_v[:, cols], axis=1, keepdims=True)
                o_v[tp, rows, cols] = (acc_v[:, cols] / total).astype(BF16)

            pl.when(i == 0)(lambda: w_enter(2))

    pl.run_scoped(
        attend,
        pltpu.VMEM((chunk, d_model), BF16),
        pltpu.VMEM((d_model, q_cols), BF16),
        pltpu.VMEM((d_model, 2 * HEAD_DIM), BF16),
        pltpu.VMEM((chunk, q_cols), BF16),
        pltpu.VMEM((chunk, HEAD_DIM), jnp.int32),
        pltpu.VMEM((Q_BLK, chunk), F32),
        pltpu.VMEM((Q_BLK, q_cols), F32),
        pltpu.VMEM((Q_BLK, q_cols), F32),
        pltpu.VMEM((Q_BLK, q_cols), F32),
    )

    def output(acc_v, y_v):
        n_tile = 512

        def multiply(k, c, store):
            shard = tp if k == 0 else peer_shard(tp, k)
            lhs = o_v[shard, piece(c), :]

            @pl.loop(0, n_cols // n_tile)
            def _(n):
                out = pl.ds(pl.multiple_of(n * n_tile, n_tile), n_tile)
                store(out, jnp.dot(lhs, w_v[shard, :, out], preferred_element_type=F32))

        own_w.wait()

        @pl.loop(0, n_pc)
        def _(c):
            def store(out, part):
                acc_v[piece(c), out] = part

            multiply(0, c, store)
            pl.when(c == 0)(lambda: o_leave(n_blk - 1))

        pl.when(mid == 0)(lambda: w_enter(3))

        for k in (1, 2, 3):
            w_arrival(k, 0).wait_recv()
            w_copy(k, 5).start()
            w_copy(k, 7).start()
            w_arrival(k, 3).wait_recv()
            w_copy(k, 2).start()
            w_copy(k, 10).start()

        @pl.loop(0, n_pc)
        def _(c):
            o_forward(1, c)
            pl.when(mid == 1)(lambda: o_forward(3, c))

        for k in (1, 2, 3):
            w_arrival(k, 1).wait_recv()
            w_copy(k, 8).start()
            w_arrival(k, 4).wait_recv()
            w_copy(k, 11).start()

        def w_finish(k):
            w_arrival(k, 2).wait_recv()
            w_copy(k, 9).start()
            w_arrival(k, 5).wait_recv()
            w_copy(k, 12).start()
            for hop in range(6, 13):
                w_arrival(k, hop).wait_recv()

        w_finish(1)

        @pl.loop(0, n_pc)
        def _(c):
            def store(out, part):
                acc_v[piece(c), out] += part

            multiply(1, c, store)

        w_finish(2)

        @pl.loop(0, n_pc)
        def _(c):
            def store(out, part):
                acc_v[piece(c), out] += part

            o_forward(2, c)
            multiply(2, c, store)

        w_finish(3)

        def y_copy(slot, c):
            return pltpu.make_async_copy(y_v.at[slot], y_hbm.at[piece(c)], y_sem.at[slot])

        @pl.loop(0, n_pc)
        def _(c):
            slot = lax.rem(c, 2)
            pl.when(mid == 0)(lambda: o_next(3, c).wait_recv())
            pl.when(c >= 2)(lambda: y_copy(slot, c - 2).wait())

            def store(out, part):
                y_v[slot, :, out] = (acc_v[piece(c), out] + part).astype(BF16)

            multiply(3, c, store)
            y_copy(slot, c).start()

        for c in (n_pc - 2, n_pc - 1):
            y_copy(c % 2, c).wait()

    pl.run_scoped(output, pltpu.VMEM((chunk, n_cols), F32), pltpu.VMEM((2, O_ROWS, n_cols), BF16))

    pl.when(cp < 2)(lambda: over(kv_copies(0, cp, cp_y), 'wait_send'))
    pl.when(core == 0)(lambda: over(kv_copies(1, cp, cp_c), 'wait_send'))
    pl.when(cp >= 2)(lambda: over(kv_copies(2, cp - 2, cp_c), 'wait_send'))
    pl.when(tp < 3)(z_up.wait_send)
    pl.when(tp > 0)(z_down.wait_send)
    for k in (1, 2, 3):
        pl.when(mid == 1)(lambda: z_next(k).wait_send())
        for hop in range(len(hops)):
            w_copy(k, hop).wait_send()

    @pl.loop(0, n_pc)
    def _(c):
        pl.when(tp < 3)(lambda: o_up(c).wait_send())
        pl.when(tp > 0)(lambda: o_down(c).wait_send())

        @pl.when(mid == 1)
        def _():
            for k in (1, 2, 3):
                o_next(k, c).wait_send()


def solution(mesh):
    any_spec = pl.BlockSpec(memory_space=pl.ANY)
    dma = pltpu.SemaphoreType.DMA

    def layer(x_loc, seg_loc, w_query, w_key, w_value, w_out):
        chunk = x_loc.shape[0]
        q_cols = w_query.shape[1]
        n_blk = chunk // Q_BLK
        n_pc = chunk // O_ROWS
        return pl.pallas_call(
            layer_kernel,
            name='layer',
            out_shape=jax.ShapeDtypeStruct((chunk, w_out.shape[1]), BF16),
            in_specs=[any_spec] * 6,
            out_specs=any_spec,
            scratch_shapes=[
                pltpu.VMEM((4,) + w_out.shape, BF16),
                pltpu.VMEM((4, chunk, q_cols), BF16),
                pltpu.VMEM((4 * chunk, 2 * HEAD_DIM), BF16),
                pltpu.VMEM((1, 4 * chunk), jnp.int32),
                dma((n_blk + 5,)), dma((3,)), dma((3,)), dma((3,)), dma((3,)), dma((5,)), dma((4,)),
                dma((3, 13)), dma((3, 13)), dma((5, n_pc)), dma((4, n_pc)), dma((2,)),
            ],
            compiler_params=pltpu.CompilerParams(collective_id=0, has_side_effects=True, vmem_limit_bytes=67043328),
        )(x_loc, seg_loc[None, :], w_query, w_key, w_value, w_out)

    return jax.shard_map(layer, mesh=mesh, in_specs=(P(('dp', 'cp'), None), P(('dp', 'cp')), P(None, 'tp'), P(None, 'tp'), P(None, 'tp'), P('tp', None)), out_specs=P(('dp', 'cp'), None), check_vma=False)
```

```python
import functools

import jax
import jax.numpy as jnp
from jax import lax
from jax.experimental import pallas as pl
from jax.experimental.pallas import tpu as pltpu
from jax.sharding import PartitionSpec as P

HEAD_DIM = 128
MESH = pl.DeviceIdType.MESH
LOG2_SCALE = (HEAD_DIM ** -0.5) * 1.4426950408889634
F32 = jnp.float32
BF16 = jnp.bfloat16

Q_BLK = 256
LOC_BLK = 512
O_ROWS = 128


def coords():
    return lax.axis_index('dp'), lax.axis_index('tp'), lax.axis_index('cp')


def greet(dp, tp, cp, mid):
    bar = pltpu.get_barrier_semaphore()

    def hello(dev):
        pl.semaphore_signal(bar, inc=1, device_id=dev, device_id_type=MESH)

    hello((1 - dp, tp, cp))
    hello((dp, tp, lax.rem(cp + 2, 4)))
    hello((dp, tp, cp + 1 - 2 * lax.rem(cp, 2)))
    pl.when(tp > 0)(lambda: hello((dp, tp - 1, cp)))
    pl.when(tp < 3)(lambda: hello((dp, tp + 1, cp)))
    pl.semaphore_wait(bar, 4 + mid)


def peer_shard(tp, k):
    if k == 1:
        return tp + 1 - 2 * lax.rem(tp, 2)
    if k == 2:
        return lax.rem(tp + 2, 4)
    return 3 - tp


def layer_kernel(x_hbm, seg_hbm, wq_hbm, wk_hbm, wv_hbm, wo_hbm, y_hbm,
                 w_v, o_v, kv_v, seg_v, wx_v,
                 load_sem, kv_send, kv_recv, seg_send, seg_recv, x_send, x_recv, z_send, z_recv, w_send, w_recv, o_send, o_recv, y_sem):
    dp, tp, cp = coords()
    mid = lax.rem((tp + 1) // 2, 2)
    core = lax.rem(cp, 2)
    chunk, d_model = x_hbm.shape
    q_cols = wq_hbm.shape[1]
    heads = q_cols // HEAD_DIM
    n_rows = wo_hbm.shape[0] // 8
    n_cols = wo_hbm.shape[1]
    half = n_cols // 2
    x_rows = d_model // 8
    wx_cols = q_cols + 2 * HEAD_DIM
    n_blk = chunk // Q_BLK
    n_pc = chunk // O_ROWS
    per_blk = Q_BLK // O_ROWS
    cp_y = lax.rem(cp + 2, 4)
    cp_c = cp + 1 - 2 * core
    dev_x, dev_y, dev_c = (1 - dp, tp, cp), (dp, tp, cp_y), (dp, tp, cp_c)

    def onward(shard):
        return tp + 1 - 2 * (shard // (tp + 1) > 0).astype(jnp.int32)

    def rows_of(dp_i, cp_i):
        return pl.ds(pl.multiple_of((dp_i * 4 + cp_i) * n_rows, 16), n_rows)

    def z_copy(slot, src, shard, to):
        return pltpu.make_async_remote_copy(src, w_v.at[shard, rows_of(dp, cp)], z_send.at[slot], z_recv.at[shard],
                                            device_id=(dp, to, cp), device_id_type=MESH)

    z_up = z_copy(0, wo_hbm.at[rows_of(dp, cp)], tp, tp + 1)
    z_down = z_copy(4, wo_hbm.at[rows_of(dp, cp)], tp, tp - 1)

    def z_next(k):
        shard = peer_shard(tp, k)
        return z_copy(k, w_v.at[shard, rows_of(dp, cp)], shard, onward(shard))

    def x_slice(dp_i, cp_i, part='ab'):
        first = (dp_i * 4 + cp_i) * x_rows + (x_rows // 2 if part == 'b' else 0)
        return pl.ds(pl.multiple_of(first, 16), x_rows if part == 'ab' else x_rows // 2)

    def wx_copies():
        rows = x_slice(dp, cp)
        out = []
        for n, (src, lo, hi) in enumerate(((wq_hbm, 0, q_cols), (wk_hbm, q_cols, q_cols + HEAD_DIM), (wv_hbm, q_cols + HEAD_DIM, wx_cols))):
            out.append(pltpu.make_async_remote_copy(src.at[rows], wx_v.at[rows, lo:hi], x_send.at[n], x_recv.at[n],
                                                    device_id=(dp, tp - 1 + 2 * (tp // 2), cp), device_id_type=MESH))
        return out

    cuts = {'a': pl.ds(0, half), 'b': pl.ds(half, half), 'ab': pl.ds(0, n_cols)}
    hops = [('x', 'own', 'a'), ('x', 'own', 'b'), ('x', 'y', 'b'), ('y', 'own', 'b'), ('y', 'own', 'a'), ('y', 'x', 'a'),
            ('c', 'own', 'ab'), ('c', 'x', 'a'), ('c', 'x', 'b'), ('c', 'd', 'b'), ('c', 'y', 'b'), ('c', 'y', 'a'), ('c', 'd', 'a')]

    def holder(name, dp_i, cp_i):
        far = lax.rem(cp_i + 2, 4)
        return {'own': (dp_i, cp_i), 'x': (1 - dp_i, cp_i), 'y': (dp_i, far), 'd': (1 - dp_i, far)}[name]

    def w_hop(k, hop, dp_i, cp_i):
        route, name, part = hops[hop]
        if k == 4:
            at = wx_v.at[x_slice(*holder(name, dp_i, cp_i), part)]
        else:
            at = w_v.at[peer_shard(tp, k), rows_of(*holder(name, dp_i, cp_i)), cuts[part]]
        dev = {'x': dev_x, 'y': dev_y, 'c': dev_c}[route]
        return pltpu.make_async_remote_copy(at, at, w_send.at[k - 1, hop], w_recv.at[k - 1, hop], device_id=dev, device_id_type=MESH)

    def w_copy(k, hop):
        return w_hop(k, hop, dp, cp)

    def w_arrival(k, hop):
        dp_i, cp_i = {'x': (1 - dp, cp), 'y': (dp, cp_y), 'c': (dp, cp_c)}[hops[hop][0]]
        return w_hop(k, hop, dp_i, cp_i)

    def w_enter(k):
        z_next(k).wait_recv()
        pl.when(mid == 1)(lambda: z_next(k).start())
        w_spread(k)

    def w_spread(k):
        for hop in (0, 3, 6, 1, 4):
            w_copy(k, hop).start()

    def w_pass_first(k):
        w_arrival(k, 0).wait_recv()
        w_copy(k, 5).start()
        w_copy(k, 7).start()
        w_arrival(k, 3).wait_recv()
        w_copy(k, 2).start()
        w_copy(k, 10).start()

    def w_pass_second(k):
        w_arrival(k, 1).wait_recv()
        w_copy(k, 8).start()
        w_arrival(k, 4).wait_recv()
        w_copy(k, 11).start()

    def w_finish(k):
        w_arrival(k, 2).wait_recv()
        w_copy(k, 9).start()
        w_arrival(k, 5).wait_recv()
        w_copy(k, 12).start()
        for hop in range(6, 13):
            w_arrival(k, hop).wait_recv()

    def piece(c):
        return pl.ds(pl.multiple_of(c * O_ROWS, O_ROWS), O_ROWS)

    def o_copy(slot, c, shard, to):
        at = o_v.at[shard, piece(c)]
        return pltpu.make_async_remote_copy(at, at, o_send.at[slot, c], o_recv.at[shard, c], device_id=(dp, to, cp), device_id_type=MESH)

    def o_own(c):
        return o_copy(0, c, tp, tp + 1 - 2 * (tp // 2))

    def o_leave(i):
        for j in range(per_blk):
            o_own(i * per_blk + j).start()

    def o_next(k, c):
        shard = peer_shard(tp, k)
        return o_copy(k, c, shard, onward(shard))

    def o_forward(k, c):
        o_next(k, c).wait_recv()
        pl.when(mid == 1)(lambda: o_next(k, c).start())

    def kv_copies(g, slot, block, to):
        rows = pl.ds(pl.multiple_of(block * chunk, chunk), chunk)
        dev = (dp, tp, to)
        kv = pltpu.make_async_remote_copy(kv_v.at[g, rows], kv_v.at[g, rows], kv_send.at[g, slot], kv_recv.at[g, slot],
                                          device_id=dev, device_id_type=MESH)
        if g == 1:
            return (kv,)
        return (kv, pltpu.make_async_remote_copy(seg_v.at[:, rows], seg_v.at[:, rows], seg_send.at[slot], seg_recv.at[slot],
            device_id=dev, device_id_type=MESH))

    def kv_leave(g):
        pl.when(cp < 2)(lambda: over(kv_copies(g, 0, cp, cp_y), 'start'))
        pl.when(core == 0)(lambda: over(kv_copies(g, 1, cp, cp_c), 'start'))

    def kv_wait(g):
        @pl.when(cp >= 2)
        def _():
            over(kv_copies(g, 0, cp - 2, cp), 'wait_recv')
            over(kv_copies(g, 2, cp - 2, cp_c), 'start')
            over(kv_copies(g, 2, cp_c - 2, cp), 'wait_recv')

        @pl.when(core == 1)
        def _():
            over(kv_copies(g, 1, cp_c, cp), 'wait_recv')

    def kv_sent(g):
        pl.when(cp < 2)(lambda: over(kv_copies(g, 0, cp, cp_y), 'wait_send'))
        pl.when(core == 0)(lambda: over(kv_copies(g, 1, cp, cp_c), 'wait_send'))
        pl.when(cp >= 2)(lambda: over(kv_copies(g, 2, cp - 2, cp_c), 'wait_send'))

    def over(copies, what):
        for copy in copies:
            getattr(copy, what)()

    own_w = pltpu.make_async_copy(wo_hbm, w_v.at[tp], load_sem.at[n_blk + 5])

    def attend(x_v, w_blk, q_v, col_v, bias_v, m_v, l_v, acc_v):
        n_w = 2 * HEAD_DIM
        own = pl.ds(pl.multiple_of(cp * chunk, chunk), chunk)
        x_loads = []
        for i in range(n_blk):
            rows = slice(i * Q_BLK, (i + 1) * Q_BLK)
            x_loads.append(pltpu.make_async_copy(x_hbm.at[rows], x_v.at[rows], load_sem.at[i]))
        seg_load = pltpu.make_async_copy(seg_hbm, seg_v.at[:, own], load_sem.at[n_blk])
        spans = [(lo, min(lo + n_w, q_cols)) for lo in range(0, q_cols, n_w)]
        w_loads = [[pltpu.make_async_copy(wk_hbm, w_blk.at[0, :, 0:HEAD_DIM], load_sem.at[n_blk + 1]),
                    pltpu.make_async_copy(wv_hbm, w_blk.at[0, :, HEAD_DIM:n_w], load_sem.at[n_blk + 2])]]
        for n, (lo, hi) in enumerate(spans):
            w_loads.append([pltpu.make_async_copy(wq_hbm.at[:, lo:hi], w_blk.at[(n + 1) % 2, :, 0:hi - lo],
                                                  load_sem.at[n_blk + 3 + (n + 1) % 2])])
        over(w_loads[0], 'start')
        over(x_loads, 'start')
        over(w_loads[1], 'start')
        seg_load.start()

        greet(dp, tp, cp, mid)
        pl.when(mid == 1)(lambda: over(wx_copies(), 'start'))
        pl.when(tp < 3)(z_up.start)
        pl.when(tp > 0)(z_down.start)

        def blk(i):
            return pl.ds(pl.multiple_of(i * Q_BLK, Q_BLK), Q_BLK)

        def own_rows(i):
            return pl.ds(pl.multiple_of(cp * chunk + i * Q_BLK, Q_BLK), Q_BLK)

        def product(i, w):
            return jnp.dot(x_v[blk(i), :], w, preferred_element_type=F32).astype(BF16)

        over(w_loads[0], 'wait')
        for i in range(n_blk):
            x_loads[i].wait()
            kv_v[0, own_rows(i), :] = product(i, w_blk[0])
        over(w_loads[2], 'start')
        seg_load.wait()
        for n, (lo, hi) in enumerate(spans):
            over(w_loads[n + 1], 'wait')

            @pl.loop(0, n_blk)
            def _(i):
                q_v[blk(i), lo:hi] = product(i, w_blk[(n + 1) % 2, :, 0:hi - lo])

            if n + 3 < len(w_loads):
                over(w_loads[n + 3], 'start')
            if n == 0:
                kv_leave(0)
        own_w.start()

        @pl.loop(0, chunk // HEAD_DIM)
        def _(i):
            ids = seg_v[0:1, pl.ds(pl.multiple_of(cp * chunk + i * HEAD_DIM, HEAD_DIM), HEAD_DIM)]
            rows = pl.ds(pl.multiple_of(i * HEAD_DIM, HEAD_DIM), HEAD_DIM)
            col_v[rows, :] = jnp.transpose(jnp.broadcast_to(ids, (HEAD_DIM, HEAD_DIM)))

        @pl.when(mid == 1)
        def _():
            w_enter(1)
            w_enter(3)

        @pl.when(mid == 0)
        def _():
            over(wx_copies(), 'wait_recv')
            w_spread(4)

        def step(g, i, key0, n_keys, first):
            keys = pl.ds(pl.multiple_of(key0, n_keys), n_keys)
            groups = n_keys // HEAD_DIM
            q_seg = col_v[blk(i), :]
            for n in range(groups):
                cols = pl.ds(pl.multiple_of(key0 + n * HEAD_DIM, HEAD_DIM), HEAD_DIM)
                ok = q_seg == seg_v[0:1, cols]
                if first:
                    q_pos = cp * chunk + i * Q_BLK + lax.broadcasted_iota(jnp.int32, (Q_BLK, HEAD_DIM), 0)
                    k_pos = key0 + n * HEAD_DIM + lax.broadcasted_iota(jnp.int32, (Q_BLK, HEAD_DIM), 1)
                    ok = ok & (q_pos >= k_pos)
                bias_v[:, n * HEAD_DIM:(n + 1) * HEAD_DIM] = jnp.where(ok, 0.0, -jnp.inf)
            k_blk = kv_v[g, keys, 0:HEAD_DIM]
            v_blk = kv_v[g, keys, HEAD_DIM:2 * HEAD_DIM]

            def scores(h):
                return lax.dot_general(q_v[blk(i), h * HEAD_DIM:(h + 1) * HEAD_DIM], k_blk, (((1,), (1,)), ((), ())),
                                       preferred_element_type=F32)

            ahead = scores(0)
            for h in range(heads):
                cols = slice(h * HEAD_DIM, (h + 1) * HEAD_DIM)
                s = ahead
                if h + 1 < heads:
                    ahead = scores(h + 1)
                s = [s[:, n * HEAD_DIM:(n + 1) * HEAD_DIM] + bias_v[:, n * HEAD_DIM:(n + 1) * HEAD_DIM] for n in range(groups)]
                top = jnp.max(functools.reduce(jnp.maximum, s), axis=1, keepdims=True)
                if first:
                    m_new = jnp.broadcast_to(top, (Q_BLK, HEAD_DIM))
                else:
                    m_old = m_v[:, cols]
                    m_new = jnp.maximum(m_old, top)
                    fade = jnp.exp2((m_old - m_new) * LOG2_SCALE)
                p = [jnp.exp2((part - m_new) * LOG2_SCALE) for part in s]
                total = functools.reduce(jnp.add, p)
                probs = jnp.concatenate([part.astype(BF16) for part in p], axis=1)
                pv = jnp.dot(probs, v_blk, preferred_element_type=F32)
                m_v[:, cols] = m_new
                if first:
                    l_v[:, cols] = total
                    acc_v[:, cols] = pv
                else:
                    l_v[:, cols] = l_v[:, cols] * fade + total
                    acc_v[:, cols] = acc_v[:, cols] * fade + pv

        per_loc = LOC_BLK // Q_BLK

        def attention(g, shard, after_first, after_block):
            @pl.loop(0, n_blk)
            def _(i):
                last = i // per_loc
                step(g, i, cp * chunk + last * LOC_BLK, LOC_BLK, True)
                after_first(i)

                @pl.loop(0, last)
                def _(j):
                    step(g, i, cp * chunk + j * LOC_BLK, LOC_BLK, False)

                pl.when(i == 0)(lambda: kv_wait(g))

                @pl.loop(0, cp)
                def _(j):
                    step(g, i, j * chunk, chunk, False)

                for h in range(heads):
                    cols = slice(h * HEAD_DIM, (h + 1) * HEAD_DIM)
                    total = jnp.sum(l_v[:, cols], axis=1, keepdims=True)
                    o_v[shard, blk(i), cols] = (acc_v[:, cols] / total).astype(BF16)
                after_block(i)

        def own_after_first(i):
            pl.when(i > 0)(lambda: o_leave(i - 1))

        def own_after_block(i):
            pl.when((i == 0) & (mid == 1))(lambda: w_enter(2))
            pl.when((i == 0) & (mid == 0))(lambda: w_pass_first(4))
            pl.when((i == 1) & (mid == 0))(lambda: w_enter(1))
            pl.when((i == 2) & (mid == 0))(lambda: w_pass_second(4))

        attention(0, tp, own_after_first, own_after_block)

        @pl.when(mid == 0)
        def _():
            w_finish(4)
            w_enter(2)

            @pl.loop(0, n_blk)
            def _(i):
                kv_v[1, own_rows(i), :] = product(i, wx_v[:, q_cols:wx_cols])

            o_leave(n_blk - 1)

            @pl.loop(0, n_blk)
            def _(i):
                q_v[blk(i), :] = product(i, wx_v[:, 0:q_cols])
                pl.when(i == 0)(lambda: kv_leave(1))

            def more_after_block(i):
                @pl.when(i == 0)
                def _():
                    w_enter(3)

                @pl.when(i == 1)
                def _():
                    w_pass_first(1)
                    w_pass_first(2)

                @pl.when(i == 2)
                def _():
                    w_pass_second(1)
                    w_pass_second(2)

            attention(1, peer_shard(tp, 1), lambda i: None, more_after_block)

    pl.run_scoped(
        attend,
        pltpu.VMEM((chunk, d_model), BF16),
        pltpu.VMEM((2, d_model, 2 * HEAD_DIM), BF16),
        pltpu.VMEM((chunk, q_cols), BF16),
        pltpu.VMEM((chunk, HEAD_DIM), jnp.int32),
        pltpu.VMEM((Q_BLK, chunk), F32),
        pltpu.VMEM((Q_BLK, q_cols), F32),
        pltpu.VMEM((Q_BLK, q_cols), F32),
        pltpu.VMEM((Q_BLK, q_cols), F32),
    )

    def output(acc_v, y_v):
        n_tile = 512

        def multiply(k, c, store):
            shard = tp if k == 0 else peer_shard(tp, k)
            lhs = o_v[shard, piece(c), :]

            @pl.loop(0, n_cols // n_tile)
            def _(n):
                out = pl.ds(pl.multiple_of(n * n_tile, n_tile), n_tile)
                store(out, jnp.dot(lhs, w_v[shard, :, out], preferred_element_type=F32))

        own_w.wait()

        @pl.when(mid == 0)
        def _():
            w_pass_first(3)
            w_pass_second(3)

        @pl.loop(0, n_pc)
        def _(c):
            def store(out, part):
                acc_v[piece(c), out] = part

            multiply(0, c, store)
            pl.when((c == 0) & (mid == 1))(lambda: o_leave(n_blk - 1))

        @pl.when(mid == 1)
        def _():
            for k in (1, 2, 3):
                w_pass_first(k)

            @pl.loop(0, n_pc)
            def _(c):
                o_forward(1, c)
                o_forward(3, c)

            for k in (1, 2, 3):
                w_pass_second(k)

        w_finish(1)

        @pl.loop(0, n_pc)
        def _(c):
            def store(out, part):
                acc_v[piece(c), out] += part

            multiply(1, c, store)

        w_finish(2)

        @pl.loop(0, n_pc)
        def _(c):
            def store(out, part):
                acc_v[piece(c), out] += part

            o_forward(2, c)
            multiply(2, c, store)

        w_finish(3)

        def y_copy(slot, c):
            return pltpu.make_async_copy(y_v.at[slot], y_hbm.at[piece(c)], y_sem.at[slot])

        @pl.loop(0, n_pc)
        def _(c):
            slot = lax.rem(c, 2)
            pl.when(mid == 0)(lambda: o_next(3, c).wait_recv())
            pl.when(c >= 2)(lambda: y_copy(slot, c - 2).wait())

            def store(out, part):
                y_v[slot, :, out] = (acc_v[piece(c), out] + part).astype(BF16)

            multiply(3, c, store)
            y_copy(slot, c).start()

        for c in (n_pc - 2, n_pc - 1):
            y_copy(c % 2, c).wait()

    pl.run_scoped(output, pltpu.VMEM((chunk, n_cols), F32), pltpu.VMEM((2, O_ROWS, n_cols), BF16))

    kv_sent(0)

    @pl.when(mid == 0)
    def _():
        kv_sent(1)
        for hop in range(len(hops)):
            w_copy(4, hop).wait_send()

    pl.when(mid == 1)(lambda: over(wx_copies(), 'wait_send'))
    pl.when(tp < 3)(z_up.wait_send)
    pl.when(tp > 0)(z_down.wait_send)
    for k in (1, 2, 3):
        pl.when(mid == 1)(lambda: z_next(k).wait_send())
        for hop in range(len(hops)):
            w_copy(k, hop).wait_send()

    @pl.loop(0, n_pc)
    def _(c):
        o_own(c).wait_send()

        @pl.when(mid == 1)
        def _():
            for k in (1, 2, 3):
                o_next(k, c).wait_send()


def solution(mesh):
    any_spec = pl.BlockSpec(memory_space=pl.ANY)
    dma = pltpu.SemaphoreType.DMA

    def layer(x_loc, seg_loc, w_query, w_key, w_value, w_out):
        chunk = x_loc.shape[0]
        q_cols = w_query.shape[1]
        n_blk = chunk // Q_BLK
        n_pc = chunk // O_ROWS
        return pl.pallas_call(
            layer_kernel,
            name='layer',
            out_shape=jax.ShapeDtypeStruct((chunk, w_out.shape[1]), BF16),
            in_specs=[any_spec] * 6,
            out_specs=any_spec,
            scratch_shapes=[
                pltpu.VMEM((4,) + w_out.shape, BF16),
                pltpu.VMEM((4, chunk, q_cols), BF16),
                pltpu.VMEM((2, 4 * chunk, 2 * HEAD_DIM), BF16),
                pltpu.VMEM((1, 4 * chunk), jnp.int32),
                pltpu.VMEM((x_loc.shape[1], q_cols + 2 * HEAD_DIM), BF16),
                dma((n_blk + 6,)), dma((2, 3)), dma((2, 3)), dma((3,)), dma((3,)), dma((3,)), dma((3,)), dma((5,)), dma((4,)),
                dma((4, 13)), dma((4, 13)), dma((5, n_pc)), dma((4, n_pc)), dma((2,)),
            ],
            compiler_params=pltpu.CompilerParams(collective_id=0, has_side_effects=True, vmem_limit_bytes=67043328),
        )(x_loc, seg_loc[None, :], w_query, w_key, w_value, w_out)

    return jax.shard_map(layer, mesh=mesh, in_specs=(P(('dp', 'cp'), None), P(('dp', 'cp')), P(None, 'tp'), P(None, 'tp'), P(None, 'tp'), P('tp', None)), out_specs=P(('dp', 'cp'), None), check_vma=False)
```

```python
import functools

import jax
import jax.numpy as jnp
from jax import lax
from jax.experimental import pallas as pl
from jax.experimental.pallas import tpu as pltpu
from jax.sharding import PartitionSpec as P

HEAD_DIM = 128
MESH = pl.DeviceIdType.MESH
LOG2_SCALE = (HEAD_DIM ** -0.5) * 1.4426950408889634
F32 = jnp.float32
BF16 = jnp.bfloat16

Q_BLK = 256
LOC_BLK = 512
O_ROWS = 128


def coords():
    return lax.axis_index('dp'), lax.axis_index('tp'), lax.axis_index('cp')


def greet(dp, tp, cp, mid):
    bar = pltpu.get_barrier_semaphore()

    def hello(dev):
        pl.semaphore_signal(bar, inc=1, device_id=dev, device_id_type=MESH)

    hello((1 - dp, tp, cp))
    hello((dp, tp, lax.rem(cp + 2, 4)))
    hello((dp, tp, cp + 1 - 2 * lax.rem(cp, 2)))
    pl.when(tp > 0)(lambda: hello((dp, tp - 1, cp)))
    pl.when(tp < 3)(lambda: hello((dp, tp + 1, cp)))
    pl.semaphore_wait(bar, 4 + mid)


def peer_shard(tp, k):
    if k == 1:
        return tp + 1 - 2 * lax.rem(tp, 2)
    if k == 2:
        return lax.rem(tp + 2, 4)
    return 3 - tp


def layer_kernel(x_hbm, seg_hbm, wq_hbm, wk_hbm, wv_hbm, wo_hbm, y_hbm,
                 w_v, o_v, kv_v, seg_v, wx_v,
                 load_sem, kv_send, kv_recv, seg_send, seg_recv, x_send, x_recv, z_send, z_recv, w_send, w_recv, o_send, o_recv, y_sem):
    dp, tp, cp = coords()
    mid = lax.rem((tp + 1) // 2, 2)
    core = lax.rem(cp, 2)
    chunk, d_model = x_hbm.shape
    q_cols = wq_hbm.shape[1]
    heads = q_cols // HEAD_DIM
    n_rows = wo_hbm.shape[0] // 8
    n_cols = wo_hbm.shape[1]
    part_a = n_cols // HEAD_DIM * 3 // 7 * HEAD_DIM
    x_rows = d_model // 8
    wx_cols = q_cols + 2 * HEAD_DIM
    n_blk = chunk // Q_BLK
    n_pc = chunk // O_ROWS
    per_blk = Q_BLK // O_ROWS
    cp_y = lax.rem(cp + 2, 4)
    cp_c = cp + 1 - 2 * core
    dev_x, dev_y, dev_c = (1 - dp, tp, cp), (dp, tp, cp_y), (dp, tp, cp_c)

    def onward(shard):
        return tp + 1 - 2 * (shard // (tp + 1) > 0).astype(jnp.int32)

    def rows_of(dp_i, cp_i):
        return pl.ds(pl.multiple_of((dp_i * 4 + cp_i) * n_rows, 16), n_rows)

    def z_copy(slot, src, shard, to):
        return pltpu.make_async_remote_copy(src, w_v.at[shard, rows_of(dp, cp)], z_send.at[slot], z_recv.at[shard],
                                            device_id=(dp, to, cp), device_id_type=MESH)

    z_up = z_copy(0, wo_hbm.at[rows_of(dp, cp)], tp, tp + 1)
    z_down = z_copy(4, wo_hbm.at[rows_of(dp, cp)], tp, tp - 1)

    def z_next(k):
        shard = peer_shard(tp, k)
        return z_copy(k, w_v.at[shard, rows_of(dp, cp)], shard, onward(shard))

    def x_slice(dp_i, cp_i, part='ab'):
        rows_a = x_rows * 3 // 7
        first = (dp_i * 4 + cp_i) * x_rows + (rows_a if part == 'b' else 0)
        return pl.ds(pl.multiple_of(first, 16), {'a': rows_a, 'b': x_rows - rows_a, 'ab': x_rows}[part])

    def wx_copies(part):
        rows = x_slice(dp, cp, part)
        first = 3 * (part == 'b')
        out = []
        for n, (src, lo, hi) in enumerate(((wq_hbm, 0, q_cols), (wk_hbm, q_cols, q_cols + HEAD_DIM), (wv_hbm, q_cols + HEAD_DIM, wx_cols))):
            out.append(pltpu.make_async_remote_copy(src.at[rows], wx_v.at[rows, lo:hi], x_send.at[first + n], x_recv.at[first + n],
                                                    device_id=(dp, tp - 1 + 2 * (tp // 2), cp), device_id_type=MESH))
        return out

    cuts = {'a': pl.ds(0, part_a), 'b': pl.ds(part_a, n_cols - part_a), 'ab': pl.ds(0, n_cols)}
    hops = [('x', 'own', 'a'), ('x', 'own', 'b'), ('x', 'y', 'b'), ('y', 'own', 'b'), ('y', 'own', 'a'), ('y', 'x', 'a'),
            ('c', 'own', 'ab'), ('c', 'x', 'a'), ('c', 'x', 'b'), ('c', 'd', 'b'), ('c', 'y', 'b'), ('c', 'y', 'a'), ('c', 'd', 'a')]

    def holder(name, dp_i, cp_i):
        far = lax.rem(cp_i + 2, 4)
        return {'own': (dp_i, cp_i), 'x': (1 - dp_i, cp_i), 'y': (dp_i, far), 'd': (1 - dp_i, far)}[name]

    def w_hop(k, hop, dp_i, cp_i):
        route, name, part = hops[hop]
        if k == 4:
            at = wx_v.at[x_slice(*holder(name, dp_i, cp_i), part)]
        else:
            at = w_v.at[peer_shard(tp, k), rows_of(*holder(name, dp_i, cp_i)), cuts[part]]
        dev = {'x': dev_x, 'y': dev_y, 'c': dev_c}[route]
        return pltpu.make_async_remote_copy(at, at, w_send.at[k - 1, hop], w_recv.at[k - 1, hop], device_id=dev, device_id_type=MESH)

    def w_copy(k, hop):
        return w_hop(k, hop, dp, cp)

    def w_arrival(k, hop):
        dp_i, cp_i = {'x': (1 - dp, cp), 'y': (dp, cp_y), 'c': (dp, cp_c)}[hops[hop][0]]
        return w_hop(k, hop, dp_i, cp_i)

    def w_arrived(k):
        z_next(k).wait_recv()
        pl.when(mid == 1)(lambda: z_next(k).start())

    def w_send_on(k, *which):
        for hop in which:
            w_copy(k, hop).start()

    def w_enter(k):
        w_arrived(k)
        w_send_on(k, 0, 3, 6, 1, 4)

    def w_relay(k, *which):
        after = {0: (5, 7), 1: (8,), 2: (9,), 3: (2, 10), 4: (11,), 5: (12,)}
        for hop in which:
            w_arrival(k, hop).wait_recv()
            w_send_on(k, *after[hop])

    def w_finish(k):
        w_relay(k, 2, 5)
        for hop in range(6, 13):
            w_arrival(k, hop).wait_recv()

    def piece(c):
        return pl.ds(pl.multiple_of(c * O_ROWS, O_ROWS), O_ROWS)

    def nth(n):
        return (n_blk - 1 - n // per_blk) * per_blk + lax.rem(n, per_blk)

    def o_copy(slot, c, shard, to):
        at = o_v.at[shard, piece(c)]
        return pltpu.make_async_remote_copy(at, at, o_send.at[slot, c], o_recv.at[shard, c], device_id=(dp, to, cp), device_id_type=MESH)

    def o_own(c):
        return o_copy(0, c, tp, tp + 1 - 2 * (tp // 2))

    def o_leave(i):
        for j in range(per_blk):
            o_own(i * per_blk + j).start()

    def o_next(k, c):
        shard = peer_shard(tp, k)
        return o_copy(k, c, shard, onward(shard))

    def o_forward(k, c):
        o_next(k, c).wait_recv()
        pl.when(mid == 1)(lambda: o_next(k, c).start())

    def kv_copies(g, slot, block, to):
        rows = pl.ds(pl.multiple_of(block * chunk, chunk), chunk)
        dev = (dp, tp, to)
        kv = pltpu.make_async_remote_copy(kv_v.at[g, rows], kv_v.at[g, rows], kv_send.at[g, slot], kv_recv.at[g, slot],
                                          device_id=dev, device_id_type=MESH)
        if g == 1:
            return (kv,)
        return (kv, pltpu.make_async_remote_copy(seg_v.at[:, rows], seg_v.at[:, rows], seg_send.at[slot], seg_recv.at[slot],
            device_id=dev, device_id_type=MESH))

    def kv_leave(g):
        pl.when(cp < 2)(lambda: over(kv_copies(g, 0, cp, cp_y), 'start'))
        pl.when(core == 0)(lambda: over(kv_copies(g, 1, cp, cp_c), 'start'))

    def kv_wait(g):
        @pl.when(cp >= 2)
        def _():
            over(kv_copies(g, 0, cp - 2, cp), 'wait_recv')
            over(kv_copies(g, 2, cp - 2, cp_c), 'start')
            over(kv_copies(g, 2, cp_c - 2, cp), 'wait_recv')

        @pl.when(core == 1)
        def _():
            over(kv_copies(g, 1, cp_c, cp), 'wait_recv')

    def kv_sent(g):
        pl.when(cp < 2)(lambda: over(kv_copies(g, 0, cp, cp_y), 'wait_send'))
        pl.when(core == 0)(lambda: over(kv_copies(g, 1, cp, cp_c), 'wait_send'))
        pl.when(cp >= 2)(lambda: over(kv_copies(g, 2, cp - 2, cp_c), 'wait_send'))

    def over(copies, what):
        for copy in copies:
            getattr(copy, what)()

    own_w = pltpu.make_async_copy(wo_hbm, w_v.at[tp], load_sem.at[n_blk + 5])

    def attend(x_v, w_blk, q_v, col_v, bias_v, m_v, l_v, acc_v):
        n_w = 2 * HEAD_DIM
        own = pl.ds(pl.multiple_of(cp * chunk, chunk), chunk)
        x_loads = []
        for i in range(n_blk):
            rows = slice(i * Q_BLK, (i + 1) * Q_BLK)
            x_loads.append(pltpu.make_async_copy(x_hbm.at[rows], x_v.at[rows], load_sem.at[i]))
        seg_load = pltpu.make_async_copy(seg_hbm, seg_v.at[:, own], load_sem.at[n_blk])
        spans = [(lo, min(lo + n_w, q_cols)) for lo in range(0, q_cols, n_w)]
        w_loads = [[pltpu.make_async_copy(wk_hbm, w_blk.at[0, :, 0:HEAD_DIM], load_sem.at[n_blk + 1]),
                    pltpu.make_async_copy(wv_hbm, w_blk.at[0, :, HEAD_DIM:n_w], load_sem.at[n_blk + 2])]]
        for n, (lo, hi) in enumerate(spans):
            w_loads.append([pltpu.make_async_copy(wq_hbm.at[:, lo:hi], w_blk.at[(n + 1) % 2, :, 0:hi - lo],
                                                  load_sem.at[n_blk + 3 + (n + 1) % 2])])
        over(w_loads[0], 'start')
        over(x_loads, 'start')
        over(w_loads[1], 'start')
        seg_load.start()

        greet(dp, tp, cp, mid)

        @pl.when(mid == 1)
        def _():
            over(wx_copies('a'), 'start')
            over(wx_copies('b'), 'start')

        pl.when(tp < 3)(z_up.start)
        pl.when(tp > 0)(z_down.start)

        def blk(i):
            return pl.ds(pl.multiple_of(i * Q_BLK, Q_BLK), Q_BLK)

        def own_rows(i):
            return pl.ds(pl.multiple_of(cp * chunk + i * Q_BLK, Q_BLK), Q_BLK)

        def product(i, w):
            return jnp.dot(x_v[blk(i), :], w, preferred_element_type=F32).astype(BF16)

        over(w_loads[0], 'wait')
        for i in range(n_blk):
            x_loads[i].wait()
            kv_v[0, own_rows(i), :] = product(i, w_blk[0])
        over(w_loads[2], 'start')
        seg_load.wait()
        for n, (lo, hi) in enumerate(spans):
            over(w_loads[n + 1], 'wait')

            @pl.loop(0, n_blk)
            def _(i):
                q_v[blk(i), lo:hi] = product(i, w_blk[(n + 1) % 2, :, 0:hi - lo])

            if n + 3 < len(w_loads):
                over(w_loads[n + 3], 'start')
            if n == 0:
                kv_leave(0)
        own_w.start()

        @pl.loop(0, chunk // HEAD_DIM)
        def _(i):
            ids = seg_v[0:1, pl.ds(pl.multiple_of(cp * chunk + i * HEAD_DIM, HEAD_DIM), HEAD_DIM)]
            rows = pl.ds(pl.multiple_of(i * HEAD_DIM, HEAD_DIM), HEAD_DIM)
            col_v[rows, :] = jnp.transpose(jnp.broadcast_to(ids, (HEAD_DIM, HEAD_DIM)))

        @pl.when(mid == 0)
        def _():
            over(wx_copies('a'), 'wait_recv')
            w_send_on(4, 0, 4)

        def step(g, i, key0, n_keys, first):
            keys = pl.ds(pl.multiple_of(key0, n_keys), n_keys)
            groups = n_keys // HEAD_DIM
            q_seg = col_v[blk(i), :]
            for n in range(groups):
                cols = pl.ds(pl.multiple_of(key0 + n * HEAD_DIM, HEAD_DIM), HEAD_DIM)
                ok = q_seg == seg_v[0:1, cols]
                if first:
                    q_pos = cp * chunk + i * Q_BLK + lax.broadcasted_iota(jnp.int32, (Q_BLK, HEAD_DIM), 0)
                    k_pos = key0 + n * HEAD_DIM + lax.broadcasted_iota(jnp.int32, (Q_BLK, HEAD_DIM), 1)
                    ok = ok & (q_pos >= k_pos)
                bias_v[:, n * HEAD_DIM:(n + 1) * HEAD_DIM] = jnp.where(ok, 0.0, -jnp.inf)
            k_blk = kv_v[g, keys, 0:HEAD_DIM]
            v_blk = kv_v[g, keys, HEAD_DIM:2 * HEAD_DIM]

            def scores(h):
                return lax.dot_general(q_v[blk(i), h * HEAD_DIM:(h + 1) * HEAD_DIM], k_blk, (((1,), (1,)), ((), ())),
                                       preferred_element_type=F32)

            ahead = scores(0)
            for h in range(heads):
                cols = slice(h * HEAD_DIM, (h + 1) * HEAD_DIM)
                s = ahead
                if h + 1 < heads:
                    ahead = scores(h + 1)
                s = [s[:, n * HEAD_DIM:(n + 1) * HEAD_DIM] + bias_v[:, n * HEAD_DIM:(n + 1) * HEAD_DIM] for n in range(groups)]
                top = jnp.max(functools.reduce(jnp.maximum, s), axis=1, keepdims=True)
                if first:
                    m_new = jnp.broadcast_to(top, (Q_BLK, HEAD_DIM))
                else:
                    m_old = m_v[:, cols]
                    m_new = jnp.maximum(m_old, top)
                    fade = jnp.exp2((m_old - m_new) * LOG2_SCALE)
                p = [jnp.exp2((part - m_new) * LOG2_SCALE) for part in s]
                total = functools.reduce(jnp.add, p)
                probs = jnp.concatenate([part.astype(BF16) for part in p], axis=1)
                pv = jnp.dot(probs, v_blk, preferred_element_type=F32)
                m_v[:, cols] = m_new
                if first:
                    l_v[:, cols] = total
                    acc_v[:, cols] = pv
                else:
                    l_v[:, cols] = l_v[:, cols] * fade + total
                    acc_v[:, cols] = acc_v[:, cols] * fade + pv

        per_loc = LOC_BLK // Q_BLK

        def attention(g, shard, after_first, inside, after_block):
            @pl.loop(0, n_blk)
            def _(t):
                i = n_blk - 1 - t
                last = i // per_loc
                step(g, i, cp * chunk + last * LOC_BLK, LOC_BLK, True)
                after_first(t)

                @pl.loop(0, last)
                def _(j):
                    step(g, i, cp * chunk + j * LOC_BLK, LOC_BLK, False)

                pl.when(t == 0)(lambda: kv_wait(g))

                @pl.loop(0, cp)
                def _(j):
                    step(g, i, j * chunk, chunk, False)
                    if inside is not None:
                        pl.when((t == 0) & (j == 0))(inside)

                if inside is not None:
                    pl.when((t == 0) & (cp == 0))(inside)
                for h in range(heads):
                    cols = slice(h * HEAD_DIM, (h + 1) * HEAD_DIM)
                    total = jnp.sum(l_v[:, cols], axis=1, keepdims=True)
                    o_v[shard, blk(i), cols] = (acc_v[:, cols] / total).astype(BF16)
                after_block(t)

        def own_after_first(t):
            pl.when(t > 0)(lambda: o_leave(n_blk - t))

        def own_inside():
            @pl.when(mid == 1)
            def _():
                w_enter(1)
                w_enter(3)

            @pl.when(mid == 0)
            def _():
                over(wx_copies('b'), 'wait_recv')
                w_send_on(4, 3, 1, 6)

        def own_after_block(t):
            pl.when((t == 1) & (mid == 1))(lambda: w_enter(2))
            pl.when((t == 0) & (mid == 0))(lambda: w_relay(4, 0, 4))

            @pl.when((t == 1) & (mid == 0))
            def _():
                w_relay(4, 3, 1)
                w_arrived(1)
                w_send_on(1, 0, 3, 6, 1)

        attention(0, tp, own_after_first, own_inside, own_after_block)

        @pl.when(mid == 0)
        def _():
            w_finish(4)

            @pl.loop(0, n_blk)
            def _(i):
                kv_v[1, own_rows(i), :] = product(i, wx_v[:, q_cols:wx_cols])

            o_leave(0)

            @pl.loop(0, n_blk)
            def _(i):
                q_v[blk(i), :] = product(i, wx_v[:, 0:q_cols])

                @pl.when(i == 0)
                def _():
                    kv_leave(1)
                    w_send_on(1, 4)
                    w_enter(2)

            def more_after_block(t):
                @pl.when(t == 0)
                def _():
                    w_relay(1, 0, 3)
                    w_enter(3)

                @pl.when(t == 1)
                def _():
                    w_relay(1, 1, 4)
                    w_relay(2, 0, 3)

                pl.when(t == 2)(lambda: w_relay(2, 1, 4))

            attention(1, peer_shard(tp, 1), lambda t: None, None, more_after_block)

    pl.run_scoped(
        attend,
        pltpu.VMEM((chunk, d_model), BF16),
        pltpu.VMEM((2, d_model, 2 * HEAD_DIM), BF16),
        pltpu.VMEM((chunk, q_cols), BF16),
        pltpu.VMEM((chunk, HEAD_DIM), jnp.int32),
        pltpu.VMEM((Q_BLK, chunk), F32),
        pltpu.VMEM((Q_BLK, q_cols), F32),
        pltpu.VMEM((Q_BLK, q_cols), F32),
        pltpu.VMEM((Q_BLK, q_cols), F32),
    )

    def output(acc_v, y_v):
        n_tile = 512

        big = 2 * Q_BLK

        def multiply(ks, rows, store):
            @pl.loop(0, n_cols // n_tile)
            def _(n):
                out = pl.ds(pl.multiple_of(n * n_tile, n_tile), n_tile)
                parts = []
                for k in ks:
                    shard = tp if k == 0 else peer_shard(tp, k)
                    parts.append(jnp.dot(o_v[shard, rows, :], w_v[shard, :, out], preferred_element_type=F32))
                store(out, functools.reduce(jnp.add, parts))

        def span(i, size):
            return pl.ds(pl.multiple_of(i * size, size), size)

        own_w.wait()

        @pl.when(mid == 1)
        def _():
            w_relay(1, 0, 3)
            o_leave(0)
            w_relay(3, 0, 3)
            w_relay(1, 1, 4)
            w_relay(3, 1, 4)

            @pl.loop(0, n_pc)
            def _(n):
                o_forward(1, nth(n))
                o_forward(3, nth(n))

            w_relay(2, 0, 3, 1, 4)

        @pl.when(mid == 0)
        def _():
            w_relay(3, 0, 3)

        w_finish(1)

        @pl.loop(0, chunk // big)
        def _(i):
            rows = span(i, big)

            def store(out, part):
                acc_v[rows, out] = part

            multiply((0, 1), rows, store)

        pl.when(mid == 0)(lambda: w_relay(3, 1, 4))
        w_finish(2)

        @pl.loop(0, chunk // big)
        def _(n):
            for j in range(big // O_ROWS):
                o_forward(2, nth(n * (big // O_ROWS) + j))
            rows = span(chunk // big - 1 - n, big)

            def store(out, part):
                acc_v[rows, out] += part

            multiply((2,), rows, store)

        w_finish(3)

        def last_shard(first, pieces, slot):
            n_out = pieces * O_ROWS
            row0 = chunk - (first + pieces) * O_ROWS if pieces > 1 else (first - (n_pc - per_blk)) * O_ROWS
            rows = pl.ds(row0, n_out)

            @pl.when(mid == 0)
            def _():
                for n in range(first, first + pieces):
                    o_next(3, nth(n)).wait_recv()

            held = pl.ds(first * O_ROWS if pieces > 1 else row0, n_out)

            def store(out, part):
                y_v[held, out] = (acc_v[rows, out] + part).astype(BF16)

            multiply((3,), rows, store)
            copy = pltpu.make_async_copy(y_v.at[held], y_hbm.at[rows], y_sem.at[slot])
            copy.start()
            return copy

        copies = [last_shard(0, n_pc // 2, 0), last_shard(n_pc // 2, per_blk, 1)]
        copies[0].wait()
        for n in range(n_pc - per_blk, n_pc):
            copies.append(last_shard(n, 1, len(copies)))
        for copy in copies[1:]:
            copy.wait()

    pl.run_scoped(output, pltpu.VMEM((chunk, n_cols), F32), pltpu.VMEM((chunk - Q_BLK, n_cols), BF16))

    kv_sent(0)

    @pl.when(mid == 0)
    def _():
        kv_sent(1)
        for hop in range(len(hops)):
            w_copy(4, hop).wait_send()

    @pl.when(mid == 1)
    def _():
        over(wx_copies('a'), 'wait_send')
        over(wx_copies('b'), 'wait_send')

    pl.when(tp < 3)(z_up.wait_send)
    pl.when(tp > 0)(z_down.wait_send)
    for k in (1, 2, 3):
        pl.when(mid == 1)(lambda: z_next(k).wait_send())
        for hop in range(len(hops)):
            w_copy(k, hop).wait_send()

    @pl.loop(0, n_pc)
    def _(c):
        o_own(c).wait_send()

        @pl.when(mid == 1)
        def _():
            for k in (1, 2, 3):
                o_next(k, c).wait_send()


def solution(mesh):
    any_spec = pl.BlockSpec(memory_space=pl.ANY)
    dma = pltpu.SemaphoreType.DMA

    def layer(x_loc, seg_loc, w_query, w_key, w_value, w_out):
        chunk = x_loc.shape[0]
        q_cols = w_query.shape[1]
        n_blk = chunk // Q_BLK
        n_pc = chunk // O_ROWS
        return pl.pallas_call(
            layer_kernel,
            name='layer',
            out_shape=jax.ShapeDtypeStruct((chunk, w_out.shape[1]), BF16),
            in_specs=[any_spec] * 6,
            out_specs=any_spec,
            scratch_shapes=[
                pltpu.VMEM((4,) + w_out.shape, BF16),
                pltpu.VMEM((4, chunk, q_cols), BF16),
                pltpu.VMEM((2, 4 * chunk, 2 * HEAD_DIM), BF16),
                pltpu.VMEM((1, 4 * chunk), jnp.int32),
                pltpu.VMEM((x_loc.shape[1], q_cols + 2 * HEAD_DIM), BF16),
                dma((n_blk + 6,)), dma((2, 3)), dma((2, 3)), dma((3,)), dma((3,)), dma((6,)), dma((6,)), dma((5,)), dma((4,)),
                dma((4, 13)), dma((4, 13)), dma((5, n_pc)), dma((4, n_pc)), dma((4,)),
            ],
            compiler_params=pltpu.CompilerParams(collective_id=0, has_side_effects=True, vmem_limit_bytes=67043328),
        )(x_loc, seg_loc[None, :], w_query, w_key, w_value, w_out)

    return jax.shard_map(layer, mesh=mesh, in_specs=(P(('dp', 'cp'), None), P(('dp', 'cp')), P(None, 'tp'), P(None, 'tp'), P(None, 'tp'), P('tp', None)), out_specs=P(('dp', 'cp'), None), check_vma=False)
```

```python
import functools

import jax
import jax.numpy as jnp
from jax import lax
from jax.experimental import pallas as pl
from jax.experimental.pallas import tpu as pltpu
from jax.sharding import PartitionSpec as P

HEAD_DIM = 128
MESH = pl.DeviceIdType.MESH
LOG2_SCALE = (HEAD_DIM ** -0.5) * 1.4426950408889634
F32 = jnp.float32
BF16 = jnp.bfloat16

Q_BLK = 256
LOC_BLK = 512
O_ROWS = 128


def coords():
    return lax.axis_index('dp'), lax.axis_index('tp'), lax.axis_index('cp')


def greet(dp, tp, cp, mid):
    bar = pltpu.get_barrier_semaphore()

    def hello(dev):
        pl.semaphore_signal(bar, inc=1, device_id=dev, device_id_type=MESH)

    hello((1 - dp, tp, cp))
    hello((dp, tp, lax.rem(cp + 2, 4)))
    hello((dp, tp, cp + 1 - 2 * lax.rem(cp, 2)))
    pl.when(tp > 0)(lambda: hello((dp, tp - 1, cp)))
    pl.when(tp < 3)(lambda: hello((dp, tp + 1, cp)))
    pl.semaphore_wait(bar, 4 + mid)


def peer_shard(tp, k):
    if k == 1:
        return tp + 1 - 2 * lax.rem(tp, 2)
    if k == 2:
        return 2 - tp // 2
    return 3 * (1 - tp // 2)


def layer_kernel(x_hbm, seg_hbm, wq_hbm, wk_hbm, wv_hbm, wo_hbm, y_hbm,
                 w_v, o_v, kv_v, seg_v, wx_v,
                 load_sem, kv_send, kv_recv, seg_send, seg_recv, x_send, x_recv, z_send, z_recv, w_send, w_recv, o_send, o_recv, y_sem):
    dp, tp, cp = coords()
    mid = lax.rem((tp + 1) // 2, 2)
    core = lax.rem(cp, 2)
    chunk, d_model = x_hbm.shape
    q_cols = wq_hbm.shape[1]
    heads = q_cols // HEAD_DIM
    n_rows = wo_hbm.shape[0] // 8
    n_cols = wo_hbm.shape[1]
    part_a = n_cols // HEAD_DIM * 3 // 7 * HEAD_DIM
    x_rows = d_model // 8
    wx_cols = q_cols + 2 * HEAD_DIM
    n_blk = chunk // Q_BLK
    n_pc = chunk // O_ROWS
    per_blk = Q_BLK // O_ROWS
    cp_y = lax.rem(cp + 2, 4)
    cp_c = cp + 1 - 2 * core
    dev_x, dev_y, dev_c = (1 - dp, tp, cp), (dp, tp, cp_y), (dp, tp, cp_c)

    def onward(shard):
        return tp + 1 - 2 * (shard // (tp + 1) > 0).astype(jnp.int32)

    def rows_of(dp_i, cp_i):
        return pl.ds(pl.multiple_of((dp_i * 4 + cp_i) * n_rows, 16), n_rows)

    def z_copy(slot, src, shard, to):
        return pltpu.make_async_remote_copy(src, w_v.at[shard, rows_of(dp, cp)], z_send.at[slot], z_recv.at[shard],
                                            device_id=(dp, to, cp), device_id_type=MESH)

    z_up = z_copy(0, wo_hbm.at[rows_of(dp, cp)], tp, tp + 1)
    z_down = z_copy(4, wo_hbm.at[rows_of(dp, cp)], tp, tp - 1)

    def z_next(k):
        shard = peer_shard(tp, k)
        return z_copy(k, w_v.at[shard, rows_of(dp, cp)], shard, onward(shard))

    def x_slice(dp_i, cp_i, part='ab'):
        rows_a = x_rows * 3 // 7
        first = (dp_i * 4 + cp_i) * x_rows + (rows_a if part == 'b' else 0)
        return pl.ds(pl.multiple_of(first, 16), {'a': rows_a, 'b': x_rows - rows_a, 'ab': x_rows}[part])

    def wx_copies(part):
        rows = x_slice(dp, cp, part)
        first = 3 * (part == 'b')
        out = []
        for n, (src, lo, hi) in enumerate(((wq_hbm, 0, q_cols), (wk_hbm, q_cols, q_cols + HEAD_DIM), (wv_hbm, q_cols + HEAD_DIM, wx_cols))):
            out.append(pltpu.make_async_remote_copy(src.at[rows], wx_v.at[rows, lo:hi], x_send.at[first + n], x_recv.at[first + n],
                                                    device_id=(dp, tp - 1 + 2 * (tp // 2), cp), device_id_type=MESH))
        return out

    cuts = {'a': pl.ds(0, part_a), 'b': pl.ds(part_a, n_cols - part_a), 'ab': pl.ds(0, n_cols)}
    hops = [('x', 'own', 'a'), ('x', 'own', 'b'), ('x', 'y', 'b'), ('y', 'own', 'b'), ('y', 'own', 'a'), ('y', 'x', 'a'),
            ('c', 'own', 'ab'), ('c', 'x', 'a'), ('c', 'x', 'b'), ('c', 'd', 'b'), ('c', 'y', 'b'), ('c', 'y', 'a'), ('c', 'd', 'a')]

    def holder(name, dp_i, cp_i):
        far = lax.rem(cp_i + 2, 4)
        return {'own': (dp_i, cp_i), 'x': (1 - dp_i, cp_i), 'y': (dp_i, far), 'd': (1 - dp_i, far)}[name]

    def w_hop(k, hop, dp_i, cp_i):
        route, name, part = hops[hop]
        if k == 4:
            at = wx_v.at[x_slice(*holder(name, dp_i, cp_i), part)]
        else:
            at = w_v.at[peer_shard(tp, k), rows_of(*holder(name, dp_i, cp_i)), cuts[part]]
        dev = {'x': dev_x, 'y': dev_y, 'c': dev_c}[route]
        return pltpu.make_async_remote_copy(at, at, w_send.at[k - 1, hop], w_recv.at[k - 1, hop], device_id=dev, device_id_type=MESH)

    def w_copy(k, hop):
        return w_hop(k, hop, dp, cp)

    def w_arrival(k, hop):
        dp_i, cp_i = {'x': (1 - dp, cp), 'y': (dp, cp_y), 'c': (dp, cp_c)}[hops[hop][0]]
        return w_hop(k, hop, dp_i, cp_i)

    def w_arrived(k):
        z_next(k).wait_recv()
        pl.when(mid == 1)(lambda: z_next(k).start())

    def w_send_on(k, *which):
        for hop in which:
            w_copy(k, hop).start()

    def w_enter(k):
        w_arrived(k)
        w_send_on(k, 0, 3, 6, 1, 4)

    def w_relay(k, *which):
        after = {0: (5, 7), 1: (8,), 2: (9,), 3: (2, 10), 4: (11,), 5: (12,)}
        for hop in which:
            w_arrival(k, hop).wait_recv()
            w_send_on(k, *after[hop])

    def w_finish(k):
        for hop in range(6, 13):
            w_arrival(k, hop).wait_recv()

    def piece(c):
        return pl.ds(pl.multiple_of(c * O_ROWS, O_ROWS), O_ROWS)

    def nth(n):
        return (n_blk - 1 - n // per_blk) * per_blk + lax.rem(n, per_blk)

    def o_copy(slot, c, shard, to):
        at = o_v.at[shard, piece(c)]
        return pltpu.make_async_remote_copy(at, at, o_send.at[slot, c], o_recv.at[shard, c], device_id=(dp, to, cp), device_id_type=MESH)

    def o_own(c):
        return o_copy(0, c, tp, tp + 1 - 2 * (tp // 2))

    def o_leave(i):
        for j in range(per_blk):
            o_own(i * per_blk + j).start()

    def o_next(k, c):
        shard = peer_shard(tp, k)
        return o_copy(k, c, shard, onward(shard))

    def o_forward(k, c):
        o_next(k, c).wait_recv()
        pl.when(mid == 1)(lambda: o_next(k, c).start())

    def kv_copies(g, slot, block, to):
        rows = pl.ds(pl.multiple_of(block * chunk, chunk), chunk)
        dev = (dp, tp, to)
        kv = pltpu.make_async_remote_copy(kv_v.at[g, rows], kv_v.at[g, rows], kv_send.at[g, slot], kv_recv.at[g, slot],
                                          device_id=dev, device_id_type=MESH)
        if g == 1:
            return (kv,)
        return (kv, pltpu.make_async_remote_copy(seg_v.at[:, rows], seg_v.at[:, rows], seg_send.at[slot], seg_recv.at[slot],
            device_id=dev, device_id_type=MESH))

    def kv_leave(g):
        pl.when(cp < 2)(lambda: over(kv_copies(g, 0, cp, cp_y), 'start'))
        pl.when(core == 0)(lambda: over(kv_copies(g, 1, cp, cp_c), 'start'))

    def kv_wait(g):
        @pl.when(cp >= 2)
        def _():
            over(kv_copies(g, 0, cp - 2, cp), 'wait_recv')
            over(kv_copies(g, 2, cp - 2, cp_c), 'start')
            over(kv_copies(g, 2, cp_c - 2, cp), 'wait_recv')

        @pl.when(core == 1)
        def _():
            over(kv_copies(g, 1, cp_c, cp), 'wait_recv')

    def kv_sent(g):
        pl.when(cp < 2)(lambda: over(kv_copies(g, 0, cp, cp_y), 'wait_send'))
        pl.when(core == 0)(lambda: over(kv_copies(g, 1, cp, cp_c), 'wait_send'))
        pl.when(cp >= 2)(lambda: over(kv_copies(g, 2, cp - 2, cp_c), 'wait_send'))

    def over(copies, what):
        for copy in copies:
            getattr(copy, what)()

    own_w = pltpu.make_async_copy(wo_hbm, w_v.at[tp], load_sem.at[n_blk + 5])

    def attend(x_v, w_blk, q_v, col_v, bias_v, m_v, l_v, acc_v):
        n_w = 2 * HEAD_DIM
        own = pl.ds(pl.multiple_of(cp * chunk, chunk), chunk)
        x_loads = []
        for i in range(n_blk):
            rows = slice(i * Q_BLK, (i + 1) * Q_BLK)
            x_loads.append(pltpu.make_async_copy(x_hbm.at[rows], x_v.at[rows], load_sem.at[i]))
        seg_load = pltpu.make_async_copy(seg_hbm, seg_v.at[:, own], load_sem.at[n_blk])
        spans = [(lo, min(lo + n_w, q_cols)) for lo in range(0, q_cols, n_w)]
        w_loads = [[pltpu.make_async_copy(wk_hbm, w_blk.at[0, :, 0:HEAD_DIM], load_sem.at[n_blk + 1]),
                    pltpu.make_async_copy(wv_hbm, w_blk.at[0, :, HEAD_DIM:n_w], load_sem.at[n_blk + 2])]]
        for n, (lo, hi) in enumerate(spans):
            w_loads.append([pltpu.make_async_copy(wq_hbm.at[:, lo:hi], w_blk.at[(n + 1) % 2, :, 0:hi - lo],
                                                  load_sem.at[n_blk + 3 + (n + 1) % 2])])
        over(w_loads[0], 'start')
        over(x_loads, 'start')
        over(w_loads[1], 'start')
        seg_load.start()

        greet(dp, tp, cp, mid)

        @pl.when(mid == 1)
        def _():
            over(wx_copies('a'), 'start')
            over(wx_copies('b'), 'start')

        pl.when(tp < 3)(z_up.start)
        pl.when(tp > 0)(z_down.start)

        def blk(i):
            return pl.ds(pl.multiple_of(i * Q_BLK, Q_BLK), Q_BLK)

        def own_rows(i):
            return pl.ds(pl.multiple_of(cp * chunk + i * Q_BLK, Q_BLK), Q_BLK)

        def product(i, w):
            return jnp.dot(x_v[blk(i), :], w, preferred_element_type=F32).astype(BF16)

        over(w_loads[0], 'wait')

        @pl.loop(0, n_blk)
        def _(i):
            pltpu.make_async_copy(x_hbm.at[blk(i)], x_v.at[blk(i)], load_sem.at[i]).wait()
            kv_v[0, own_rows(i), :] = product(i, w_blk[0])

        over(w_loads[2], 'start')
        seg_load.wait()
        for n, (lo, hi) in enumerate(spans):
            over(w_loads[n + 1], 'wait')

            @pl.loop(0, n_blk)
            def _(i):
                q_v[blk(i), lo:hi] = product(i, w_blk[(n + 1) % 2, :, 0:hi - lo])
                if n == 0:
                    pl.when(i == 0)(lambda: kv_leave(0))

            if n + 3 < len(w_loads):
                over(w_loads[n + 3], 'start')
        own_w.start()

        @pl.loop(0, chunk // HEAD_DIM)
        def _(i):
            ids = seg_v[0:1, pl.ds(pl.multiple_of(cp * chunk + i * HEAD_DIM, HEAD_DIM), HEAD_DIM)]
            rows = pl.ds(pl.multiple_of(i * HEAD_DIM, HEAD_DIM), HEAD_DIM)
            col_v[rows, :] = jnp.transpose(jnp.broadcast_to(ids, (HEAD_DIM, HEAD_DIM)))

        @pl.when(mid == 0)
        def _():
            over(wx_copies('a'), 'wait_recv')
            w_send_on(4, 0, 4)

        def step(g, i, key0, n_keys, first):
            keys = pl.ds(pl.multiple_of(key0, n_keys), n_keys)
            groups = n_keys // HEAD_DIM
            q_seg = col_v[blk(i), :]
            for n in range(groups):
                cols = pl.ds(pl.multiple_of(key0 + n * HEAD_DIM, HEAD_DIM), HEAD_DIM)
                ok = q_seg == seg_v[0:1, cols]
                if first:
                    q_pos = cp * chunk + i * Q_BLK + lax.broadcasted_iota(jnp.int32, (Q_BLK, HEAD_DIM), 0)
                    k_pos = key0 + n * HEAD_DIM + lax.broadcasted_iota(jnp.int32, (Q_BLK, HEAD_DIM), 1)
                    ok = ok & (q_pos >= k_pos)
                bias_v[:, n * HEAD_DIM:(n + 1) * HEAD_DIM] = jnp.where(ok, 0.0, -jnp.inf)
            k_blk = kv_v[g, keys, 0:HEAD_DIM]
            v_blk = kv_v[g, keys, HEAD_DIM:2 * HEAD_DIM]

            def scores(h):
                return lax.dot_general(q_v[blk(i), h * HEAD_DIM:(h + 1) * HEAD_DIM], k_blk, (((1,), (1,)), ((), ())),
                                       preferred_element_type=F32)

            ahead = scores(0)
            for h in range(heads):
                cols = slice(h * HEAD_DIM, (h + 1) * HEAD_DIM)
                s = ahead
                if h + 1 < heads:
                    ahead = scores(h + 1)
                s = [s[:, n * HEAD_DIM:(n + 1) * HEAD_DIM] + bias_v[:, n * HEAD_DIM:(n + 1) * HEAD_DIM] for n in range(groups)]
                top = jnp.max(functools.reduce(jnp.maximum, s), axis=1, keepdims=True)
                if first:
                    m_new = jnp.broadcast_to(top, (Q_BLK, HEAD_DIM))
                else:
                    m_old = m_v[:, cols]
                    m_new = jnp.maximum(m_old, top)
                    fade = jnp.exp2((m_old - m_new) * LOG2_SCALE)
                p = [jnp.exp2((part - m_new) * LOG2_SCALE) for part in s]
                total = functools.reduce(jnp.add, p)
                probs = jnp.concatenate([part.astype(BF16) for part in p], axis=1)
                pv = jnp.dot(probs, v_blk, preferred_element_type=F32)
                m_v[:, cols] = m_new
                if first:
                    l_v[:, cols] = total
                    acc_v[:, cols] = pv
                else:
                    l_v[:, cols] = l_v[:, cols] * fade + total
                    acc_v[:, cols] = acc_v[:, cols] * fade + pv

        per_loc = LOC_BLK // Q_BLK

        def attention(g, shard, after_first, inside, after_block):
            @pl.loop(0, n_blk)
            def _(t):
                i = n_blk - 1 - t
                last = i // per_loc
                step(g, i, cp * chunk + last * LOC_BLK, LOC_BLK, True)
                after_first(t)

                @pl.loop(0, last)
                def _(j):
                    step(g, i, cp * chunk + j * LOC_BLK, LOC_BLK, False)

                pl.when(t == 0)(lambda: kv_wait(g))

                @pl.loop(0, cp)
                def _(j):
                    step(g, i, j * chunk, chunk, False)
                    if inside is not None:
                        pl.when((t == 0) & (j == 0))(inside)

                if inside is not None:
                    pl.when((t == 0) & (cp == 0))(inside)
                for h in range(heads):
                    cols = slice(h * HEAD_DIM, (h + 1) * HEAD_DIM)
                    total = jnp.sum(l_v[:, cols], axis=1, keepdims=True)
                    o_v[shard, blk(i), cols] = (acc_v[:, cols] / total).astype(BF16)
                after_block(t)

        def own_after_first(t):
            pl.when(t > 0)(lambda: o_leave(n_blk - t))
            pl.when((t == 3) & (mid == 0))(lambda: w_relay(4, 2, 5))

        def own_inside():
            @pl.when(mid == 1)
            def _():
                w_enter(1)
                w_enter(2)

            @pl.when(mid == 0)
            def _():
                over(wx_copies('b'), 'wait_recv')
                w_send_on(4, 3, 1, 6)

        def own_after_block(t):
            pl.when((t == 1) & (mid == 1))(lambda: w_enter(3))
            pl.when((t == 0) & (mid == 0))(lambda: w_relay(4, 0, 4))

            @pl.when((t == 1) & (mid == 0))
            def _():
                w_relay(4, 3, 1)
                w_arrived(1)
                w_send_on(1, 0, 3, 6, 1, 4)

        attention(0, tp, own_after_first, own_inside, own_after_block)

        @pl.when(mid == 0)
        def _():
            w_finish(4)

            @pl.loop(0, n_blk)
            def _(i):
                kv_v[1, own_rows(i), :] = product(i, wx_v[:, q_cols:wx_cols])

            o_leave(0)

            @pl.loop(0, n_blk)
            def _(i):
                q_v[blk(i), :] = product(i, wx_v[:, 0:q_cols])

                @pl.when(i == 0)
                def _():
                    kv_leave(1)
                    w_relay(1, 0, 3)
                    w_enter(2)

            def more_after_first(t):
                pl.when(t == 2)(lambda: w_relay(1, 2, 5))

            def more_after_block(t):
                @pl.when(t == 0)
                def _():
                    w_relay(1, 1, 4)
                    w_enter(3)

                pl.when(t == 1)(lambda: w_relay(2, 0, 3))
                pl.when(t == 2)(lambda: w_relay(2, 1, 4))

            attention(1, peer_shard(tp, 1), more_after_first, None, more_after_block)

    pl.run_scoped(
        attend,
        pltpu.VMEM((chunk, d_model), BF16),
        pltpu.VMEM((2, d_model, 2 * HEAD_DIM), BF16),
        pltpu.VMEM((chunk, q_cols), BF16),
        pltpu.VMEM((chunk, HEAD_DIM), jnp.int32),
        pltpu.VMEM((Q_BLK, chunk), F32),
        pltpu.VMEM((Q_BLK, q_cols), F32),
        pltpu.VMEM((Q_BLK, q_cols), F32),
        pltpu.VMEM((Q_BLK, q_cols), F32),
    )

    def output(acc_v, y_v):
        n_tile = 256

        def multiply(ks, rows, width, store, between):
            @pl.loop(0, n_cols // width)
            def _(n):
                out = pl.ds(pl.multiple_of(n * width, width), width)
                parts = []
                for k in ks:
                    shard = tp if k == 0 else peer_shard(tp, k)
                    parts.append(jnp.dot(o_v[shard, rows, :], w_v[shard, :, out], preferred_element_type=F32))
                store(out, functools.reduce(jnp.add, parts))
                if between is not None:
                    between(n)

        own_w.wait()

        @pl.when(mid == 1)
        def _():
            w_relay(1, 0, 3)
            o_leave(0)
            w_relay(2, 0, 3)
            w_relay(1, 1, 4)
            w_relay(2, 1, 4)

            @pl.loop(0, n_pc)
            def _(n):
                o_forward(1, nth(n))
                o_forward(2, nth(n))

            w_relay(3, 0, 3, 1, 4)
            w_relay(1, 2, 5)

        pl.when(mid == 0)(lambda: w_relay(3, 0))
        w_finish(1)

        def during_first(n):
            pl.when((n == 4) & (mid == 0))(lambda: w_relay(3, 3))

            @pl.when(n == 8)
            def _():
                w_relay(2, 2, 5)
                pl.when(mid == 0)(lambda: w_relay(3, 1))

            pl.when((n == 11) & (mid == 0))(lambda: w_relay(3, 4))

        def during_second(n):
            pl.when(n == 9)(lambda: w_relay(3, 2, 5))

        def begin(out, part):
            acc_v[:, out] = part

        def add(out, part):
            acc_v[:, out] += part

        multiply((0, 1), slice(None), n_tile, begin, during_first)
        w_finish(2)

        @pl.loop(0, n_pc)
        def _(n):
            pl.when(mid == 0)(lambda: o_next(2, nth(n)).wait_recv())
            pl.when((mid == 1) & (n < n_pc // 2))(lambda: o_forward(3, nth(n)))

        multiply((2,), slice(None), n_tile, add, during_second)
        w_finish(3)

        @pl.when(mid == 1)
        def _():
            @pl.loop(n_pc // 2, n_pc)
            def _(n):
                o_forward(3, nth(n))

        def last_shard(first, pieces, slot):
            n_out = pieces * O_ROWS
            row0 = chunk - (first + pieces) * O_ROWS if pieces > 1 else (first - (n_pc - per_blk)) * O_ROWS
            rows = pl.ds(row0, n_out)

            @pl.when(mid == 0)
            def _():
                for n in range(first, first + pieces):
                    o_next(3, nth(n)).wait_recv()

            held = pl.ds(first * O_ROWS if pieces > 1 else row0, n_out)

            def store(out, part):
                y_v[held, out] = (acc_v[rows, out] + part).astype(BF16)

            multiply((3,), rows, 2 * n_tile, store, None)
            copy = pltpu.make_async_copy(y_v.at[held], y_hbm.at[rows], y_sem.at[slot])
            copy.start()
            return copy

        copies = [last_shard(0, n_pc // 2, 0), last_shard(n_pc // 2, per_blk, 1)]
        copies[0].wait()
        for n in range(n_pc - per_blk, n_pc):
            copies.append(last_shard(n, 1, len(copies)))
        for copy in copies[1:]:
            copy.wait()

    pl.run_scoped(output, pltpu.VMEM((chunk, n_cols), F32), pltpu.VMEM((chunk - Q_BLK, n_cols), BF16))

    kv_sent(0)

    @pl.when(mid == 0)
    def _():
        kv_sent(1)
        for hop in range(len(hops)):
            w_copy(4, hop).wait_send()

    @pl.when(mid == 1)
    def _():
        over(wx_copies('a'), 'wait_send')
        over(wx_copies('b'), 'wait_send')

    pl.when(tp < 3)(z_up.wait_send)
    pl.when(tp > 0)(z_down.wait_send)
    for k in (1, 2, 3):
        pl.when(mid == 1)(lambda: z_next(k).wait_send())
        for hop in range(len(hops)):
            w_copy(k, hop).wait_send()

    @pl.loop(0, n_pc)
    def _(c):
        o_own(c).wait_send()

        @pl.when(mid == 1)
        def _():
            for k in (1, 2, 3):
                o_next(k, c).wait_send()


def solution(mesh):
    any_spec = pl.BlockSpec(memory_space=pl.ANY)
    dma = pltpu.SemaphoreType.DMA

    def layer(x_loc, seg_loc, w_query, w_key, w_value, w_out):
        chunk = x_loc.shape[0]
        q_cols = w_query.shape[1]
        n_blk = chunk // Q_BLK
        n_pc = chunk // O_ROWS
        return pl.pallas_call(
            layer_kernel,
            name='layer',
            out_shape=jax.ShapeDtypeStruct((chunk, w_out.shape[1]), BF16),
            in_specs=[any_spec] * 6,
            out_specs=any_spec,
            scratch_shapes=[
                pltpu.VMEM((4,) + w_out.shape, BF16),
                pltpu.VMEM((4, chunk, q_cols), BF16),
                pltpu.VMEM((2, 4 * chunk, 2 * HEAD_DIM), BF16),
                pltpu.VMEM((1, 4 * chunk), jnp.int32),
                pltpu.VMEM((x_loc.shape[1], q_cols + 2 * HEAD_DIM), BF16),
                dma((n_blk + 6,)), dma((2, 3)), dma((2, 3)), dma((3,)), dma((3,)), dma((6,)), dma((6,)), dma((5,)), dma((4,)),
                dma((4, 13)), dma((4, 13)), dma((5, n_pc)), dma((4, n_pc)), dma((4,)),
            ],
            compiler_params=pltpu.CompilerParams(collective_id=0, has_side_effects=True, vmem_limit_bytes=67043328),
        )(x_loc, seg_loc[None, :], w_query, w_key, w_value, w_out)

    return jax.shard_map(layer, mesh=mesh, in_specs=(P(('dp', 'cp'), None), P(('dp', 'cp')), P(None, 'tp'), P(None, 'tp'), P(None, 'tp'), P('tp', None)), out_specs=P(('dp', 'cp'), None), check_vma=False)
```

```python
import functools

import jax
import jax.numpy as jnp
from jax import lax
from jax.experimental import pallas as pl
from jax.experimental.pallas import tpu as pltpu
from jax.sharding import PartitionSpec as P

HEAD_DIM = 128
MESH = pl.DeviceIdType.MESH
LOG2_SCALE = (HEAD_DIM ** -0.5) * 1.4426950408889634
F32 = jnp.float32
BF16 = jnp.bfloat16

Q_BLK = 256
LOC_BLK = 512
O_ROWS = 128


def coords():
    return lax.axis_index('dp'), lax.axis_index('tp'), lax.axis_index('cp')


def greet(dp, tp, cp, mid):
    bar = pltpu.get_barrier_semaphore()

    def hello(dev):
        pl.semaphore_signal(bar, inc=1, device_id=dev, device_id_type=MESH)

    hello((1 - dp, tp, cp))
    hello((dp, tp, lax.rem(cp + 2, 4)))
    hello((dp, tp, cp + 1 - 2 * lax.rem(cp, 2)))
    pl.when(tp > 0)(lambda: hello((dp, tp - 1, cp)))
    pl.when(tp < 3)(lambda: hello((dp, tp + 1, cp)))
    pl.semaphore_wait(bar, 4 + mid)


def peer_shard(tp, k):
    if k == 1:
        return tp + 1 - 2 * lax.rem(tp, 2)
    if k == 2:
        return 2 - tp // 2
    return 3 * (1 - tp // 2)


def layer_kernel(x_hbm, seg_hbm, wq_hbm, wk_hbm, wv_hbm, wo_hbm, y_ref,
                 w_v, o_v, kv_v, seg_v,
                 load_sem, kv_send, kv_recv, seg_send, seg_recv, x_send, x_recv, z_send, z_recv, w_send, w_recv, o_send, o_recv):
    dp, tp, cp = coords()
    mid = lax.rem((tp + 1) // 2, 2)
    core = lax.rem(cp, 2)
    chunk, d_model = x_hbm.shape
    q_cols = wq_hbm.shape[1]
    heads = q_cols // HEAD_DIM
    n_rows = wo_hbm.shape[0] // 8
    n_cols = wo_hbm.shape[1]
    part_a = n_cols // HEAD_DIM * 3 // 7 * HEAD_DIM
    x_rows = d_model // 8
    wx_cols = q_cols + 2 * HEAD_DIM
    n_blk = chunk // Q_BLK
    n_pc = chunk // O_ROWS
    per_blk = Q_BLK // O_ROWS
    cp_y = lax.rem(cp + 2, 4)
    cp_c = cp + 1 - 2 * core
    dev_x, dev_y, dev_c = (1 - dp, tp, cp), (dp, tp, cp_y), (dp, tp, cp_c)

    def onward(shard):
        return tp + 1 - 2 * (shard // (tp + 1) > 0).astype(jnp.int32)

    def rows_of(dp_i, cp_i):
        return pl.ds(pl.multiple_of((dp_i * 4 + cp_i) * n_rows, 16), n_rows)

    def z_copy(slot, src, shard, to):
        return pltpu.make_async_remote_copy(src, w_v.at[shard, rows_of(dp, cp)], z_send.at[slot], z_recv.at[shard],
                                            device_id=(dp, to, cp), device_id_type=MESH)

    z_up = z_copy(0, wo_hbm.at[rows_of(dp, cp)], tp, tp + 1)
    z_down = z_copy(4, wo_hbm.at[rows_of(dp, cp)], tp, tp - 1)

    def z_next(k):
        shard = peer_shard(tp, k)
        return z_copy(k, w_v.at[shard, rows_of(dp, cp)], shard, onward(shard))

    def x_slice(dp_i, cp_i, part='ab'):
        rows_a = x_rows * 3 // 7
        first = (dp_i * 4 + cp_i) * x_rows + (rows_a if part == 'b' else 0)
        return pl.ds(pl.multiple_of(first, 16), {'a': rows_a, 'b': x_rows - rows_a, 'ab': x_rows}[part])

    def wx_copies(wx_v, part):
        rows = x_slice(dp, cp, part)
        first = 3 * (part == 'b')
        out = []
        for n, (src, lo, hi) in enumerate(((wq_hbm, 0, q_cols), (wk_hbm, q_cols, q_cols + HEAD_DIM), (wv_hbm, q_cols + HEAD_DIM, wx_cols))):
            out.append(pltpu.make_async_remote_copy(src.at[rows], wx_v.at[rows, lo:hi], x_send.at[first + n], x_recv.at[first + n],
                                                    device_id=(dp, tp - 1 + 2 * (tp // 2), cp), device_id_type=MESH))
        return out

    cuts = {'a': pl.ds(0, part_a), 'b': pl.ds(part_a, n_cols - part_a), 'ab': pl.ds(0, n_cols)}
    hops = [('x', 'own', 'a'), ('x', 'own', 'b'), ('x', 'y', 'b'), ('y', 'own', 'b'), ('y', 'own', 'a'), ('y', 'x', 'a'),
            ('c', 'own', 'ab'), ('c', 'x', 'a'), ('c', 'x', 'b'), ('c', 'd', 'b'), ('c', 'y', 'b'), ('c', 'y', 'a'), ('c', 'd', 'a')]

    def holder(name, dp_i, cp_i):
        far = lax.rem(cp_i + 2, 4)
        return {'own': (dp_i, cp_i), 'x': (1 - dp_i, cp_i), 'y': (dp_i, far), 'd': (1 - dp_i, far)}[name]

    wx = []

    def w_hop(k, hop, dp_i, cp_i):
        route, name, part = hops[hop]
        if k == 4:
            at = wx[0].at[x_slice(*holder(name, dp_i, cp_i), part)]
        else:
            at = w_v.at[peer_shard(tp, k), rows_of(*holder(name, dp_i, cp_i)), cuts[part]]
        dev = {'x': dev_x, 'y': dev_y, 'c': dev_c}[route]
        return pltpu.make_async_remote_copy(at, at, w_send.at[k - 1, hop], w_recv.at[k - 1, hop], device_id=dev, device_id_type=MESH)

    def w_copy(k, hop):
        return w_hop(k, hop, dp, cp)

    def w_arrival(k, hop):
        dp_i, cp_i = {'x': (1 - dp, cp), 'y': (dp, cp_y), 'c': (dp, cp_c)}[hops[hop][0]]
        return w_hop(k, hop, dp_i, cp_i)

    def w_arrived(k):
        z_next(k).wait_recv()
        pl.when(mid == 1)(lambda: z_next(k).start())

    def w_send_on(k, *which):
        for hop in which:
            w_copy(k, hop).start()

    def w_enter(k):
        w_arrived(k)
        w_send_on(k, 0, 3, 6, 1, 4)

    def w_relay(k, *which):
        after = {0: (5, 7), 1: (8,), 2: (9,), 3: (2, 10), 4: (11,), 5: (12,)}
        for hop in which:
            w_arrival(k, hop).wait_recv()
            w_send_on(k, *after[hop])

    def w_finish(k):
        for hop in range(6, 13):
            w_arrival(k, hop).wait_recv()

    def piece(c):
        return pl.ds(pl.multiple_of(c * O_ROWS, O_ROWS), O_ROWS)

    def nth(n):
        return (n_blk - 1 - n // per_blk) * per_blk + lax.rem(n, per_blk)

    def o_copy(slot, c, shard, to):
        at = o_v.at[shard, piece(c)]
        return pltpu.make_async_remote_copy(at, at, o_send.at[slot, c], o_recv.at[shard, c], device_id=(dp, to, cp), device_id_type=MESH)

    def o_own(c):
        return o_copy(0, c, tp, tp + 1 - 2 * (tp // 2))

    def o_leave(i):
        for j in range(per_blk):
            o_own(i * per_blk + j).start()

    def o_next(k, c):
        shard = peer_shard(tp, k)
        return o_copy(k, c, shard, onward(shard))

    def o_forward(k, c):
        o_next(k, c).wait_recv()
        pl.when(mid == 1)(lambda: o_next(k, c).start())

    def kv_copies(g, slot, block, to):
        rows = pl.ds(pl.multiple_of(block * chunk, chunk), chunk)
        dev = (dp, tp, to)
        kv = pltpu.make_async_remote_copy(kv_v.at[g, rows], kv_v.at[g, rows], kv_send.at[g, slot], kv_recv.at[g, slot],
                                          device_id=dev, device_id_type=MESH)
        if g == 1:
            return (kv,)
        return (kv, pltpu.make_async_remote_copy(seg_v.at[:, rows], seg_v.at[:, rows], seg_send.at[slot], seg_recv.at[slot],
            device_id=dev, device_id_type=MESH))

    def kv_leave(g):
        pl.when(cp < 2)(lambda: over(kv_copies(g, 0, cp, cp_y), 'start'))
        pl.when(core == 0)(lambda: over(kv_copies(g, 1, cp, cp_c), 'start'))

    def kv_wait(g):
        @pl.when(cp >= 2)
        def _():
            over(kv_copies(g, 0, cp - 2, cp), 'wait_recv')
            over(kv_copies(g, 2, cp - 2, cp_c), 'start')
            over(kv_copies(g, 2, cp_c - 2, cp), 'wait_recv')

        @pl.when(core == 1)
        def _():
            over(kv_copies(g, 1, cp_c, cp), 'wait_recv')

    def kv_sent(g):
        pl.when(cp < 2)(lambda: over(kv_copies(g, 0, cp, cp_y), 'wait_send'))
        pl.when(core == 0)(lambda: over(kv_copies(g, 1, cp, cp_c), 'wait_send'))
        pl.when(cp >= 2)(lambda: over(kv_copies(g, 2, cp - 2, cp_c), 'wait_send'))

    def over(copies, what):
        for copy in copies:
            getattr(copy, what)()

    own_w = pltpu.make_async_copy(wo_hbm, w_v.at[tp], load_sem.at[n_blk + 5])

    def attend(wx_v, w_blk, q_v, col_v, bias_v, m_v, l_v, acc_v):
        wx.append(wx_v)
        x_v = y_ref
        n_w = 2 * HEAD_DIM
        own = pl.ds(pl.multiple_of(cp * chunk, chunk), chunk)
        x_loads = []
        for i in range(n_blk):
            rows = slice(i * Q_BLK, (i + 1) * Q_BLK)
            x_loads.append(pltpu.make_async_copy(x_hbm.at[rows], x_v.at[rows], load_sem.at[i]))
        seg_load = pltpu.make_async_copy(seg_hbm, seg_v.at[:, own], load_sem.at[n_blk])
        spans = [(lo, min(lo + n_w, q_cols)) for lo in range(0, q_cols, n_w)]
        w_loads = [[pltpu.make_async_copy(wk_hbm, w_blk.at[0, :, 0:HEAD_DIM], load_sem.at[n_blk + 1]),
                    pltpu.make_async_copy(wv_hbm, w_blk.at[0, :, HEAD_DIM:n_w], load_sem.at[n_blk + 2])]]
        for n, (lo, hi) in enumerate(spans):
            w_loads.append([pltpu.make_async_copy(wq_hbm.at[:, lo:hi], w_blk.at[(n + 1) % 2, :, 0:hi - lo],
                                                  load_sem.at[n_blk + 3 + (n + 1) % 2])])
        over(w_loads[0], 'start')
        over(x_loads, 'start')
        over(w_loads[1], 'start')
        seg_load.start()

        greet(dp, tp, cp, mid)

        @pl.when(mid == 1)
        def _():
            over(wx_copies(wx_v, 'a'), 'start')
            over(wx_copies(wx_v, 'b'), 'start')

        pl.when(tp < 3)(z_up.start)
        pl.when(tp > 0)(z_down.start)

        def blk(i):
            return pl.ds(pl.multiple_of(i * Q_BLK, Q_BLK), Q_BLK)

        def own_rows(i):
            return pl.ds(pl.multiple_of(cp * chunk + i * Q_BLK, Q_BLK), Q_BLK)

        def product(i, w):
            return jnp.dot(x_v[blk(i), :], w, preferred_element_type=F32).astype(BF16)

        over(w_loads[0], 'wait')

        @pl.loop(0, n_blk)
        def _(i):
            pltpu.make_async_copy(x_hbm.at[blk(i)], x_v.at[blk(i)], load_sem.at[i]).wait()
            kv_v[0, own_rows(i), :] = product(i, w_blk[0])

        over(w_loads[2], 'start')
        seg_load.wait()
        for n, (lo, hi) in enumerate(spans):
            over(w_loads[n + 1], 'wait')

            @pl.loop(0, n_blk)
            def _(i):
                q_v[blk(i), lo:hi] = product(i, w_blk[(n + 1) % 2, :, 0:hi - lo])
                if n == 0:
                    pl.when(i == 0)(lambda: kv_leave(0))

            if n + 3 < len(w_loads):
                over(w_loads[n + 3], 'start')
        own_w.start()

        @pl.loop(0, chunk // HEAD_DIM)
        def _(i):
            ids = seg_v[0:1, pl.ds(pl.multiple_of(cp * chunk + i * HEAD_DIM, HEAD_DIM), HEAD_DIM)]
            rows = pl.ds(pl.multiple_of(i * HEAD_DIM, HEAD_DIM), HEAD_DIM)
            col_v[rows, :] = jnp.transpose(jnp.broadcast_to(ids, (HEAD_DIM, HEAD_DIM)))

        @pl.when(mid == 0)
        def _():
            over(wx_copies(wx_v, 'a'), 'wait_recv')
            w_send_on(4, 0, 4)

        def step(g, i, key0, n_keys, first):
            keys = pl.ds(pl.multiple_of(key0, n_keys), n_keys)
            groups = n_keys // HEAD_DIM
            q_seg = col_v[blk(i), :]
            for n in range(groups):
                cols = pl.ds(pl.multiple_of(key0 + n * HEAD_DIM, HEAD_DIM), HEAD_DIM)
                ok = q_seg == seg_v[0:1, cols]
                if first:
                    q_pos = cp * chunk + i * Q_BLK + lax.broadcasted_iota(jnp.int32, (Q_BLK, HEAD_DIM), 0)
                    k_pos = key0 + n * HEAD_DIM + lax.broadcasted_iota(jnp.int32, (Q_BLK, HEAD_DIM), 1)
                    ok = ok & (q_pos >= k_pos)
                bias_v[:, n * HEAD_DIM:(n + 1) * HEAD_DIM] = jnp.where(ok, 0.0, -jnp.inf)
            k_blk = kv_v[g, keys, 0:HEAD_DIM]
            v_blk = kv_v[g, keys, HEAD_DIM:2 * HEAD_DIM]

            def scores(h):
                return lax.dot_general(q_v[blk(i), h * HEAD_DIM:(h + 1) * HEAD_DIM], k_blk, (((1,), (1,)), ((), ())),
                                       preferred_element_type=F32)

            ahead = scores(0)
            for h in range(heads):
                cols = slice(h * HEAD_DIM, (h + 1) * HEAD_DIM)
                s = ahead
                if h + 1 < heads:
                    ahead = scores(h + 1)
                s = [s[:, n * HEAD_DIM:(n + 1) * HEAD_DIM] + bias_v[:, n * HEAD_DIM:(n + 1) * HEAD_DIM] for n in range(groups)]
                top = jnp.max(functools.reduce(jnp.maximum, s), axis=1, keepdims=True)
                if first:
                    m_new = jnp.broadcast_to(top, (Q_BLK, HEAD_DIM))
                else:
                    m_old = m_v[:, cols]
                    m_new = jnp.maximum(m_old, top)
                    fade = jnp.exp2((m_old - m_new) * LOG2_SCALE)
                p = [jnp.exp2((part - m_new) * LOG2_SCALE) for part in s]
                total = functools.reduce(jnp.add, p)
                probs = jnp.concatenate([part.astype(BF16) for part in p], axis=1)
                pv = jnp.dot(probs, v_blk, preferred_element_type=F32)
                m_v[:, cols] = m_new
                if first:
                    l_v[:, cols] = total
                    acc_v[:, cols] = pv
                else:
                    l_v[:, cols] = l_v[:, cols] * fade + total
                    acc_v[:, cols] = acc_v[:, cols] * fade + pv

        per_loc = LOC_BLK // Q_BLK

        def attention(g, shard, after_first, inside, after_block):
            @pl.loop(0, n_blk)
            def _(t):
                i = n_blk - 1 - t
                last = i // per_loc
                step(g, i, cp * chunk + last * LOC_BLK, LOC_BLK, True)
                after_first(t)

                @pl.loop(0, last)
                def _(j):
                    step(g, i, cp * chunk + j * LOC_BLK, LOC_BLK, False)

                pl.when(t == 0)(lambda: kv_wait(g))

                @pl.loop(0, cp)
                def _(j):
                    step(g, i, j * chunk, chunk, False)
                    if inside is not None:
                        pl.when((t == 0) & (j == 0))(inside)

                if inside is not None:
                    pl.when((t == 0) & (cp == 0))(inside)
                for h in range(heads):
                    cols = slice(h * HEAD_DIM, (h + 1) * HEAD_DIM)
                    total = jnp.sum(l_v[:, cols], axis=1, keepdims=True)
                    o_v[shard, blk(i), cols] = (acc_v[:, cols] / total).astype(BF16)
                after_block(t)

        def own_after_first(t):
            pl.when(t > 0)(lambda: o_leave(n_blk - t))
            pl.when((t == 3) & (mid == 0))(lambda: w_relay(4, 2, 5))

        def own_inside():
            @pl.when(mid == 1)
            def _():
                w_enter(1)
                w_enter(2)

            @pl.when(mid == 0)
            def _():
                over(wx_copies(wx_v, 'b'), 'wait_recv')
                w_send_on(4, 3, 1, 6)

        def own_after_block(t):
            pl.when((t == 1) & (mid == 1))(lambda: w_enter(3))
            pl.when((t == 0) & (mid == 0))(lambda: w_relay(4, 0, 4))

            @pl.when((t == 1) & (mid == 0))
            def _():
                w_relay(4, 3, 1)
                w_arrived(1)
                w_send_on(1, 0, 3, 6, 1, 4)

        attention(0, tp, own_after_first, own_inside, own_after_block)

        @pl.when(mid == 0)
        def _():
            w_finish(4)

            @pl.loop(0, n_blk)
            def _(i):
                kv_v[1, own_rows(i), :] = product(i, wx_v[:, q_cols:wx_cols])

            o_leave(0)

            @pl.loop(0, n_blk)
            def _(i):
                q_v[blk(i), :] = product(i, wx_v[:, 0:q_cols])

                @pl.when(i == 0)
                def _():
                    kv_leave(1)
                    w_relay(1, 0, 3)
                    w_enter(2)

            def more_after_first(t):
                pl.when(t == 2)(lambda: w_relay(1, 2, 5))

            def more_after_block(t):
                @pl.when(t == 0)
                def _():
                    w_relay(1, 1, 4)
                    w_enter(3)

                pl.when(t == 1)(lambda: w_relay(2, 0, 3))
                pl.when(t == 2)(lambda: w_relay(2, 1, 4))

            attention(1, peer_shard(tp, 1), more_after_first, None, more_after_block)
            for hop in range(len(hops)):
                w_copy(4, hop).wait_send()

        @pl.when(mid == 1)
        def _():
            over(wx_copies(wx_v, 'a'), 'wait_send')
            over(wx_copies(wx_v, 'b'), 'wait_send')

    pl.run_scoped(
        attend,
        pltpu.VMEM((d_model, wx_cols), BF16),
        pltpu.VMEM((2, d_model, 2 * HEAD_DIM), BF16),
        pltpu.VMEM((chunk, q_cols), BF16),
        pltpu.VMEM((chunk, HEAD_DIM), jnp.int32),
        pltpu.VMEM((Q_BLK, chunk), F32),
        pltpu.VMEM((Q_BLK, q_cols), F32),
        pltpu.VMEM((Q_BLK, q_cols), F32),
        pltpu.VMEM((Q_BLK, q_cols), F32),
    )

    def output(acc_v):
        n_tile = 256

        def multiply(ks, rows, width, store, between):
            @pl.loop(0, n_cols // width)
            def _(n):
                out = pl.ds(pl.multiple_of(n * width, width), width)
                parts = []
                for k in ks:
                    shard = tp if k == 0 else peer_shard(tp, k)
                    parts.append(jnp.dot(o_v[shard, rows, :], w_v[shard, :, out], preferred_element_type=F32))
                store(out, functools.reduce(jnp.add, parts))
                if between is not None:
                    between(n)

        own_w.wait()

        @pl.when(mid == 1)
        def _():
            w_relay(1, 0, 3)
            o_leave(0)
            w_relay(2, 0, 3)
            w_relay(1, 1, 4)
            w_relay(2, 1, 4)

            @pl.loop(0, n_pc)
            def _(n):
                o_forward(1, nth(n))
                o_forward(2, nth(n))

            w_relay(3, 0, 3, 1, 4)
            w_relay(1, 2, 5)

        pl.when(mid == 0)(lambda: w_relay(3, 0))
        w_finish(1)

        def during_first(n):
            pl.when((n == 4) & (mid == 0))(lambda: w_relay(3, 3))

            @pl.when(n == 8)
            def _():
                w_relay(2, 2, 5)
                pl.when(mid == 0)(lambda: w_relay(3, 1))

            pl.when((n == 11) & (mid == 0))(lambda: w_relay(3, 4))

        def during_second(n):
            pl.when(n == 9)(lambda: w_relay(3, 2, 5))

        def begin(out, part):
            acc_v[:, out] = part

        def add(out, part):
            acc_v[:, out] += part

        multiply((0, 1), slice(None), n_tile, begin, during_first)
        w_finish(2)

        @pl.loop(0, n_pc)
        def _(n):
            pl.when(mid == 0)(lambda: o_next(2, nth(n)).wait_recv())
            pl.when((mid == 1) & (n < n_pc // 2))(lambda: o_forward(3, nth(n)))

        multiply((2,), slice(None), n_tile, add, during_second)
        w_finish(3)

        @pl.when(mid == 1)
        def _():
            @pl.loop(n_pc // 2, n_pc)
            def _(n):
                o_forward(3, nth(n))

        def last_shard(first, pieces):
            row0 = chunk - (first + pieces) * O_ROWS if pieces > 1 else (first - (n_pc - per_blk)) * O_ROWS
            rows = pl.ds(row0, pieces * O_ROWS)

            @pl.when(mid == 0)
            def _():
                for n in range(first, first + pieces):
                    o_next(3, nth(n)).wait_recv()

            def store(out, part):
                y_ref[rows, out] = (acc_v[rows, out] + part).astype(BF16)

            multiply((3,), rows, 2 * n_tile, store, None)

        last_shard(0, n_pc // 2)
        last_shard(n_pc // 2, per_blk)
        for n in range(n_pc - per_blk, n_pc):
            last_shard(n, 1)

    pl.run_scoped(output, pltpu.VMEM((chunk, n_cols), F32))

    kv_sent(0)

    pl.when(mid == 0)(lambda: kv_sent(1))
    pl.when(tp < 3)(z_up.wait_send)
    pl.when(tp > 0)(z_down.wait_send)
    for k in (1, 2, 3):
        pl.when(mid == 1)(lambda: z_next(k).wait_send())
        for hop in range(len(hops)):
            w_copy(k, hop).wait_send()

    @pl.loop(0, n_pc)
    def _(c):
        o_own(c).wait_send()

        @pl.when(mid == 1)
        def _():
            for k in (1, 2, 3):
                o_next(k, c).wait_send()


def solution(mesh):
    any_spec = pl.BlockSpec(memory_space=pl.ANY)
    dma = pltpu.SemaphoreType.DMA

    def layer(x_loc, seg_loc, w_query, w_key, w_value, w_out):
        chunk = x_loc.shape[0]
        q_cols = w_query.shape[1]
        n_blk = chunk // Q_BLK
        n_pc = chunk // O_ROWS
        return pl.pallas_call(
            layer_kernel,
            name='layer',
            out_shape=pltpu.VMEM((chunk, w_out.shape[1]), BF16),
            in_specs=[any_spec] * 6,
            out_specs=pl.BlockSpec(memory_space=pltpu.VMEM),
            scratch_shapes=[
                pltpu.VMEM((4,) + w_out.shape, BF16),
                pltpu.VMEM((4, chunk, q_cols), BF16),
                pltpu.VMEM((2, 4 * chunk, 2 * HEAD_DIM), BF16),
                pltpu.VMEM((1, 4 * chunk), jnp.int32),
                dma((n_blk + 6,)), dma((2, 3)), dma((2, 3)), dma((3,)), dma((3,)), dma((6,)), dma((6,)), dma((5,)), dma((4,)),
                dma((4, 13)), dma((4, 13)), dma((5, n_pc)), dma((4, n_pc)),
            ],
            compiler_params=pltpu.CompilerParams(collective_id=0, has_side_effects=True, vmem_limit_bytes=59600000),
        )(x_loc, seg_loc[None, :], w_query, w_key, w_value, w_out)

    return jax.shard_map(layer, mesh=mesh, in_specs=(P(('dp', 'cp'), None), P(('dp', 'cp')), P(None, 'tp'), P(None, 'tp'), P(None, 'tp'), P('tp', None)), out_specs=P(('dp', 'cp'), None), check_vma=False)
```

```python
import functools

import jax
import jax.numpy as jnp
from jax import lax
from jax.experimental import pallas as pl
from jax.experimental.pallas import tpu as pltpu
from jax.sharding import PartitionSpec as P

HEAD_DIM = 128
MESH = pl.DeviceIdType.MESH
LOG2_SCALE = (HEAD_DIM ** -0.5) * 1.4426950408889634
F32 = jnp.float32
BF16 = jnp.bfloat16

Q_BLK = 256
LOC_BLK = 512
O_ROWS = 128


def coords():
    return lax.axis_index('dp'), lax.axis_index('tp'), lax.axis_index('cp')


def greet(dp, tp, cp, mid):
    bar = pltpu.get_barrier_semaphore()

    def hello(dev):
        pl.semaphore_signal(bar, inc=1, device_id=dev, device_id_type=MESH)

    hello((1 - dp, tp, cp))
    hello((dp, tp, lax.rem(cp + 2, 4)))
    hello((dp, tp, cp + 1 - 2 * lax.rem(cp, 2)))
    pl.when(tp > 0)(lambda: hello((dp, tp - 1, cp)))
    pl.when(tp < 3)(lambda: hello((dp, tp + 1, cp)))
    pl.semaphore_wait(bar, 4 + mid)


def peer_shard(tp, k):
    if k == 1:
        return tp + 1 - 2 * lax.rem(tp, 2)
    if k == 2:
        return 2 - tp // 2
    return 3 * (1 - tp // 2)


def layer_kernel(x_hbm, seg_hbm, wq_hbm, wk_hbm, wv_hbm, wo_hbm, y_ref,
                 w_v, o_v, kv_v, seg_v,
                 load_sem, kv_send, kv_recv, seg_send, seg_recv, x_send, x_recv, z_send, z_recv, w_send, w_recv, o_send, o_recv):
    dp, tp, cp = coords()
    mid = lax.rem((tp + 1) // 2, 2)
    core = lax.rem(cp, 2)
    chunk, d_model = x_hbm.shape
    q_cols = wq_hbm.shape[1]
    heads = q_cols // HEAD_DIM
    n_rows = wo_hbm.shape[0] // 8
    n_cols = wo_hbm.shape[1]
    part_a = n_cols // HEAD_DIM * 3 // 7 * HEAD_DIM
    x_rows = d_model // 8
    wx_cols = q_cols + 2 * HEAD_DIM
    n_blk = chunk // Q_BLK
    n_pc = chunk // O_ROWS
    per_blk = Q_BLK // O_ROWS
    cp_y = lax.rem(cp + 2, 4)
    cp_c = cp + 1 - 2 * core
    dev_x, dev_y, dev_c = (1 - dp, tp, cp), (dp, tp, cp_y), (dp, tp, cp_c)

    def onward(shard):
        return tp + 1 - 2 * (shard // (tp + 1) > 0).astype(jnp.int32)

    def rows_of(dp_i, cp_i):
        return pl.ds(pl.multiple_of((dp_i * 4 + cp_i) * n_rows, 16), n_rows)

    def z_copy(slot, src, shard, to):
        return pltpu.make_async_remote_copy(src, w_v.at[shard, rows_of(dp, cp)], z_send.at[slot], z_recv.at[shard],
                                            device_id=(dp, to, cp), device_id_type=MESH)

    z_up = z_copy(0, wo_hbm.at[rows_of(dp, cp)], tp, tp + 1)
    z_down = z_copy(4, wo_hbm.at[rows_of(dp, cp)], tp, tp - 1)

    def z_next(k):
        shard = peer_shard(tp, k)
        return z_copy(k, w_v.at[shard, rows_of(dp, cp)], shard, onward(shard))

    def x_slice(dp_i, cp_i, part='ab'):
        rows_a = x_rows * 3 // 7
        first = (dp_i * 4 + cp_i) * x_rows + (rows_a if part == 'b' else 0)
        return pl.ds(pl.multiple_of(first, 16), {'a': rows_a, 'b': x_rows - rows_a, 'ab': x_rows}[part])

    def wx_copies(wx_v, part):
        rows = x_slice(dp, cp, part)
        first = 3 * (part == 'b')
        out = []
        for n, (src, lo, hi) in enumerate(((wq_hbm, 0, q_cols), (wk_hbm, q_cols, q_cols + HEAD_DIM), (wv_hbm, q_cols + HEAD_DIM, wx_cols))):
            out.append(pltpu.make_async_remote_copy(src.at[rows], wx_v.at[rows, lo:hi], x_send.at[first + n], x_recv.at[first + n],
                                                    device_id=(dp, tp - 1 + 2 * (tp // 2), cp), device_id_type=MESH))
        return out

    cuts = {'a': pl.ds(0, part_a), 'b': pl.ds(part_a, n_cols - part_a), 'ab': pl.ds(0, n_cols)}
    hops = [('x', 'own', 'a'), ('x', 'own', 'b'), ('x', 'y', 'b'), ('y', 'own', 'b'), ('y', 'own', 'a'), ('y', 'x', 'a'),
            ('c', 'own', 'ab'), ('c', 'x', 'a'), ('c', 'x', 'b'), ('c', 'd', 'b'), ('c', 'y', 'b'), ('c', 'y', 'a'), ('c', 'd', 'a')]

    def holder(name, dp_i, cp_i):
        far = lax.rem(cp_i + 2, 4)
        return {'own': (dp_i, cp_i), 'x': (1 - dp_i, cp_i), 'y': (dp_i, far), 'd': (1 - dp_i, far)}[name]

    wx = []

    def w_hop(k, hop, dp_i, cp_i):
        route, name, part = hops[hop]
        if k == 4:
            at = wx[0].at[x_slice(*holder(name, dp_i, cp_i), part)]
        else:
            at = w_v.at[peer_shard(tp, k), rows_of(*holder(name, dp_i, cp_i)), cuts[part]]
        dev = {'x': dev_x, 'y': dev_y, 'c': dev_c}[route]
        return pltpu.make_async_remote_copy(at, at, w_send.at[k - 1], w_recv.at[k - 1, min(hop, 6)], device_id=dev, device_id_type=MESH)

    def w_copy(k, hop):
        return w_hop(k, hop, dp, cp)

    def w_arrival(k, hop):
        dp_i, cp_i = {'x': (1 - dp, cp), 'y': (dp, cp_y), 'c': (dp, cp_c)}[hops[hop][0]]
        return w_hop(k, hop, dp_i, cp_i)

    def w_arrived(k):
        z_next(k).wait_recv()
        pl.when(mid == 1)(lambda: z_next(k).start())

    def w_send_on(k, *which):
        for hop in which:
            w_copy(k, hop).start()

    def w_enter(k):
        w_arrived(k)
        w_send_on(k, 0, 3, 6, 1, 4)

    def w_relay(k, *which):
        after = {0: (5, 7), 1: (8,), 2: (9,), 3: (2, 10), 4: (11,), 5: (12,)}
        for hop in which:
            w_arrival(k, hop).wait_recv()
            w_send_on(k, *after[hop])

    def w_bulk(k, slices):
        at = wx[0].at[0:slices * x_rows] if k == 4 else w_v.at[peer_shard(tp, k), 0:slices * n_rows]
        return pltpu.make_async_remote_copy(at, at, w_send.at[k - 1], w_recv.at[k - 1, 6], device_id=dev_c, device_id_type=MESH)

    def w_finish(k):
        w_bulk(k, 4).wait_recv()

    def piece(c):
        return pl.ds(pl.multiple_of(c * O_ROWS, O_ROWS), O_ROWS)

    def nth(n):
        return (n_blk - 1 - n // per_blk) * per_blk + lax.rem(n, per_blk)

    def o_copy(slot, c, shard, to):
        at = o_v.at[shard, piece(c)]
        return pltpu.make_async_remote_copy(at, at, o_send.at[slot], o_recv.at[shard, c], device_id=(dp, to, cp), device_id_type=MESH)

    def o_own(c):
        return o_copy(0, c, tp, tp + 1 - 2 * (tp // 2))

    def o_leave(i):
        for j in range(per_blk):
            o_own(i * per_blk + j).start()

    def o_next(k, c):
        shard = peer_shard(tp, k)
        return o_copy(k, c, shard, onward(shard))

    def o_forward(k, c):
        o_next(k, c).wait_recv()
        pl.when(mid == 1)(lambda: o_next(k, c).start())

    def kv_copies(g, slot, block, to):
        rows = pl.ds(pl.multiple_of(block * chunk, chunk), chunk)
        dev = (dp, tp, to)
        kv = pltpu.make_async_remote_copy(kv_v.at[g, rows], kv_v.at[g, rows], kv_send.at[g, slot], kv_recv.at[g, slot],
                                          device_id=dev, device_id_type=MESH)
        if g == 1:
            return (kv,)
        return (kv, pltpu.make_async_remote_copy(seg_v.at[:, rows], seg_v.at[:, rows], seg_send.at[slot], seg_recv.at[slot],
            device_id=dev, device_id_type=MESH))

    def kv_leave(g):
        pl.when(cp < 2)(lambda: over(kv_copies(g, 0, cp, cp_y), 'start'))
        pl.when(core == 0)(lambda: over(kv_copies(g, 1, cp, cp_c), 'start'))

    def kv_wait(g):
        @pl.when(cp >= 2)
        def _():
            over(kv_copies(g, 0, cp - 2, cp), 'wait_recv')
            over(kv_copies(g, 2, cp - 2, cp_c), 'start')
            over(kv_copies(g, 2, cp_c - 2, cp), 'wait_recv')

        @pl.when(core == 1)
        def _():
            over(kv_copies(g, 1, cp_c, cp), 'wait_recv')

    def kv_sent(g):
        pl.when(cp < 2)(lambda: over(kv_copies(g, 0, cp, cp_y), 'wait_send'))
        pl.when(core == 0)(lambda: over(kv_copies(g, 1, cp, cp_c), 'wait_send'))
        pl.when(cp >= 2)(lambda: over(kv_copies(g, 2, cp - 2, cp_c), 'wait_send'))

    def over(copies, what):
        for copy in copies:
            getattr(copy, what)()

    own_w = pltpu.make_async_copy(wo_hbm, w_v.at[tp], load_sem.at[n_blk + 5])

    def attend(wx_v, w_blk, q_v, col_v, bias_v, m_v, l_v, acc_v):
        wx.append(wx_v)
        x_v = y_ref
        n_w = 2 * HEAD_DIM
        own = pl.ds(pl.multiple_of(cp * chunk, chunk), chunk)
        x_loads = []
        for i in range(n_blk):
            rows = slice(i * Q_BLK, (i + 1) * Q_BLK)
            x_loads.append(pltpu.make_async_copy(x_hbm.at[rows], x_v.at[rows], load_sem.at[i]))
        seg_load = pltpu.make_async_copy(seg_hbm, seg_v.at[:, own], load_sem.at[n_blk])
        spans = [(lo, min(lo + n_w, q_cols)) for lo in range(0, q_cols, n_w)]
        w_loads = [[pltpu.make_async_copy(wk_hbm, w_blk.at[0, :, 0:HEAD_DIM], load_sem.at[n_blk + 1]),
                    pltpu.make_async_copy(wv_hbm, w_blk.at[0, :, HEAD_DIM:n_w], load_sem.at[n_blk + 2])]]
        for n, (lo, hi) in enumerate(spans):
            w_loads.append([pltpu.make_async_copy(wq_hbm.at[:, lo:hi], w_blk.at[(n + 1) % 2, :, 0:hi - lo],
                                                  load_sem.at[n_blk + 3 + (n + 1) % 2])])
        over(w_loads[0], 'start')
        over(x_loads, 'start')
        over(w_loads[1], 'start')
        seg_load.start()

        greet(dp, tp, cp, mid)

        @pl.when(mid == 1)
        def _():
            over(wx_copies(wx_v, 'a'), 'start')
            over(wx_copies(wx_v, 'b'), 'start')

        pl.when(tp < 3)(z_up.start)
        pl.when(tp > 0)(z_down.start)

        def blk(i):
            return pl.ds(pl.multiple_of(i * Q_BLK, Q_BLK), Q_BLK)

        def own_rows(i):
            return pl.ds(pl.multiple_of(cp * chunk + i * Q_BLK, Q_BLK), Q_BLK)

        def product(i, w):
            return jnp.dot(x_v[blk(i), :], w, preferred_element_type=F32).astype(BF16)

        over(w_loads[0], 'wait')

        @pl.loop(0, n_blk)
        def _(i):
            pltpu.make_async_copy(x_hbm.at[blk(i)], x_v.at[blk(i)], load_sem.at[i]).wait()
            kv_v[0, own_rows(i), :] = product(i, w_blk[0])

        over(w_loads[2], 'start')
        seg_load.wait()
        for n, (lo, hi) in enumerate(spans):
            over(w_loads[n + 1], 'wait')

            @pl.loop(0, n_blk)
            def _(i):
                q_v[blk(i), lo:hi] = product(i, w_blk[(n + 1) % 2, :, 0:hi - lo])
                if n == 0:
                    pl.when(i == 0)(lambda: kv_leave(0))

            if n + 3 < len(w_loads):
                over(w_loads[n + 3], 'start')
        own_w.start()

        @pl.loop(0, chunk // HEAD_DIM)
        def _(i):
            ids = seg_v[0:1, pl.ds(pl.multiple_of(cp * chunk + i * HEAD_DIM, HEAD_DIM), HEAD_DIM)]
            rows = pl.ds(pl.multiple_of(i * HEAD_DIM, HEAD_DIM), HEAD_DIM)
            col_v[rows, :] = jnp.transpose(jnp.broadcast_to(ids, (HEAD_DIM, HEAD_DIM)))

        @pl.when(mid == 0)
        def _():
            over(wx_copies(wx_v, 'a'), 'wait_recv')
            w_send_on(4, 0, 4)

        def step(g, i, key0, n_keys, first):
            keys = pl.ds(pl.multiple_of(key0, n_keys), n_keys)
            groups = n_keys // HEAD_DIM
            q_seg = col_v[blk(i), :]
            for n in range(groups):
                cols = pl.ds(pl.multiple_of(key0 + n * HEAD_DIM, HEAD_DIM), HEAD_DIM)
                ok = q_seg == seg_v[0:1, cols]
                if first:
                    q_pos = cp * chunk + i * Q_BLK + lax.broadcasted_iota(jnp.int32, (Q_BLK, HEAD_DIM), 0)
                    k_pos = key0 + n * HEAD_DIM + lax.broadcasted_iota(jnp.int32, (Q_BLK, HEAD_DIM), 1)
                    ok = ok & (q_pos >= k_pos)
                bias_v[:, n * HEAD_DIM:(n + 1) * HEAD_DIM] = jnp.where(ok, 0.0, -jnp.inf)
            k_blk = kv_v[g, keys, 0:HEAD_DIM]
            v_blk = kv_v[g, keys, HEAD_DIM:2 * HEAD_DIM]

            def scores(h):
                return lax.dot_general(q_v[blk(i), h * HEAD_DIM:(h + 1) * HEAD_DIM], k_blk, (((1,), (1,)), ((), ())),
                                       preferred_element_type=F32)

            ahead = scores(0)
            for h in range(heads):
                cols = slice(h * HEAD_DIM, (h + 1) * HEAD_DIM)
                s = ahead
                if h + 1 < heads:
                    ahead = scores(h + 1)
                s = [s[:, n * HEAD_DIM:(n + 1) * HEAD_DIM] + bias_v[:, n * HEAD_DIM:(n + 1) * HEAD_DIM] for n in range(groups)]
                top = jnp.max(functools.reduce(jnp.maximum, s), axis=1, keepdims=True)
                if first:
                    m_new = jnp.broadcast_to(top, (Q_BLK, HEAD_DIM))
                else:
                    m_old = m_v[:, cols]
                    m_new = jnp.maximum(m_old, top)
                    fade = jnp.exp2((m_old - m_new) * LOG2_SCALE)
                p = [jnp.exp2((part - m_new) * LOG2_SCALE) for part in s]
                total = functools.reduce(jnp.add, p)
                probs = jnp.concatenate([part.astype(BF16) for part in p], axis=1)
                pv = jnp.dot(probs, v_blk, preferred_element_type=F32)
                m_v[:, cols] = m_new
                if first:
                    l_v[:, cols] = total
                    acc_v[:, cols] = pv
                else:
                    l_v[:, cols] = l_v[:, cols] * fade + total
                    acc_v[:, cols] = acc_v[:, cols] * fade + pv

        per_loc = LOC_BLK // Q_BLK

        def attention(g, shard, after_first, inside, after_block):
            @pl.loop(0, n_blk)
            def _(t):
                i = n_blk - 1 - t
                last = i // per_loc
                odd = lax.rem(i, per_loc)
                pl.when(odd == 1)(lambda: step(g, i, cp * chunk + last * LOC_BLK, LOC_BLK, True))
                pl.when(odd == 0)(lambda: step(g, i, cp * chunk + i * Q_BLK, Q_BLK, True))
                after_first(t)

                @pl.loop(0, last)
                def _(j):
                    step(g, i, cp * chunk + j * LOC_BLK, LOC_BLK, False)

                pl.when(t == 0)(lambda: kv_wait(g))

                @pl.loop(0, cp)
                def _(j):
                    step(g, i, j * chunk, chunk, False)
                    if inside is not None:
                        pl.when((t == 0) & (j == 0))(inside)

                if inside is not None:
                    pl.when((t == 0) & (cp == 0))(inside)
                for h in range(heads):
                    cols = slice(h * HEAD_DIM, (h + 1) * HEAD_DIM)
                    total = jnp.sum(l_v[:, cols], axis=1, keepdims=True)
                    o_v[shard, blk(i), cols] = (acc_v[:, cols] / total).astype(BF16)
                after_block(t)

        def own_after_first(t):
            pl.when(t > 0)(lambda: o_leave(n_blk - t))
            pl.when((t == 3) & (mid == 0))(lambda: w_relay(4, 2, 5))

        def own_inside():
            @pl.when(mid == 1)
            def _():
                w_enter(1)
                w_enter(2)

            @pl.when(mid == 0)
            def _():
                over(wx_copies(wx_v, 'b'), 'wait_recv')
                w_send_on(4, 3, 1, 6)

        def own_after_block(t):
            pl.when((t == 1) & (mid == 1))(lambda: w_enter(3))
            pl.when((t == 0) & (mid == 0))(lambda: w_relay(4, 0, 4))

            @pl.when((t == 1) & (mid == 0))
            def _():
                w_relay(4, 3, 1)
                w_arrived(1)
                w_send_on(1, 0, 3, 6, 1, 4)

        attention(0, tp, own_after_first, own_inside, own_after_block)

        @pl.when(mid == 0)
        def _():
            w_finish(4)

            @pl.loop(0, n_blk)
            def _(i):
                kv_v[1, own_rows(i), :] = product(i, wx_v[:, q_cols:wx_cols])

            o_leave(0)

            @pl.loop(0, n_blk)
            def _(i):
                q_v[blk(i), :] = product(i, wx_v[:, 0:q_cols])

                @pl.when(i == 0)
                def _():
                    kv_leave(1)
                    w_relay(1, 0, 3)
                    w_enter(2)

            def more_after_first(t):
                pl.when(t == 2)(lambda: w_relay(1, 2, 5))

            def more_after_block(t):
                @pl.when(t == 0)
                def _():
                    w_relay(1, 1, 4)
                    w_enter(3)

                pl.when(t == 1)(lambda: w_relay(2, 0, 3))
                pl.when(t == 2)(lambda: w_relay(2, 1, 4))

            attention(1, peer_shard(tp, 1), more_after_first, None, more_after_block)
            w_bulk(4, 7).wait_send()

        @pl.when(mid == 1)
        def _():
            over(wx_copies(wx_v, 'a'), 'wait_send')
            over(wx_copies(wx_v, 'b'), 'wait_send')

    pl.run_scoped(
        attend,
        pltpu.VMEM((d_model, wx_cols), BF16),
        pltpu.VMEM((2, d_model, 2 * HEAD_DIM), BF16),
        pltpu.VMEM((chunk, q_cols), BF16),
        pltpu.VMEM((chunk, HEAD_DIM), jnp.int32),
        pltpu.VMEM((Q_BLK, chunk), F32),
        pltpu.VMEM((Q_BLK, q_cols), F32),
        pltpu.VMEM((Q_BLK, q_cols), F32),
        pltpu.VMEM((Q_BLK, q_cols), F32),
    )

    def output(acc_v):
        n_tile = 256

        def multiply(ks, rows, width, store, between):
            @pl.loop(0, n_cols // width)
            def _(n):
                out = pl.ds(pl.multiple_of(n * width, width), width)
                parts = []
                for k in ks:
                    shard = tp if k == 0 else peer_shard(tp, k)
                    parts.append(jnp.dot(o_v[shard, rows, :], w_v[shard, :, out], preferred_element_type=F32))
                store(out, functools.reduce(jnp.add, parts))
                if between is not None:
                    between(n)

        own_w.wait()

        @pl.when(mid == 1)
        def _():
            w_relay(1, 0, 3)
            o_leave(0)
            w_relay(2, 0, 3)
            w_relay(1, 1, 4)
            w_relay(2, 1, 4)

            @pl.loop(0, n_pc)
            def _(n):
                o_forward(1, nth(n))
                o_forward(2, nth(n))

            w_relay(3, 0, 3, 1, 4)
            w_relay(1, 2, 5)

        pl.when(mid == 0)(lambda: w_relay(3, 0))
        w_finish(1)

        def during_first(n):
            pl.when((n == 4) & (mid == 0))(lambda: w_relay(3, 3))

            @pl.when(n == 8)
            def _():
                w_relay(2, 2, 5)
                pl.when(mid == 0)(lambda: w_relay(3, 1))

            pl.when((n == 11) & (mid == 0))(lambda: w_relay(3, 4))

        def during_second(n):
            pl.when(n == 9)(lambda: w_relay(3, 2, 5))

        def begin(out, part):
            acc_v[:, out] = part

        def add(out, part):
            acc_v[:, out] += part

        multiply((0, 1), slice(None), n_tile, begin, during_first)
        w_finish(2)

        @pl.loop(0, n_pc)
        def _(n):
            pl.when(mid == 0)(lambda: o_next(2, nth(n)).wait_recv())
            pl.when((mid == 1) & (n < n_pc // 2))(lambda: o_forward(3, nth(n)))

        multiply((2,), slice(None), n_tile, add, during_second)
        w_finish(3)

        @pl.when(mid == 1)
        def _():
            @pl.loop(n_pc // 2, n_pc)
            def _(n):
                o_forward(3, nth(n))

        def last_shard(first, pieces):
            row0 = chunk - (first + pieces) * O_ROWS if pieces > 1 else (first - (n_pc - per_blk)) * O_ROWS
            rows = pl.ds(row0, pieces * O_ROWS)

            @pl.when(mid == 0)
            def _():
                for n in range(first, first + pieces):
                    o_next(3, nth(n)).wait_recv()

            def store(out, part):
                y_ref[rows, out] = (acc_v[rows, out] + part).astype(BF16)

            multiply((3,), rows, 2 * n_tile, store, None)

        last_shard(0, n_pc // 2)
        last_shard(n_pc // 2, per_blk)
        for n in range(n_pc - per_blk, n_pc):
            last_shard(n, 1)

    pl.run_scoped(output, pltpu.VMEM((chunk, n_cols), F32))

    kv_sent(0)

    pl.when(mid == 0)(lambda: kv_sent(1))
    pl.when(tp < 3)(z_up.wait_send)
    pl.when(tp > 0)(z_down.wait_send)
    for k in (1, 2, 3):
        pl.when(mid == 1)(lambda: z_next(k).wait_send())
        w_bulk(k, 7).wait_send()

    def o_sent(slot, shard):
        at = o_v.at[shard]
        pltpu.make_async_remote_copy(at, at, o_send.at[slot], o_recv.at[shard, 0], device_id=dev_c, device_id_type=MESH).wait_send()

    o_sent(0, tp)

    @pl.when(mid == 1)
    def _():
        for k in (1, 2, 3):
            o_sent(k, peer_shard(tp, k))


def solution(mesh):
    any_spec = pl.BlockSpec(memory_space=pl.ANY)
    dma = pltpu.SemaphoreType.DMA

    def layer(x_loc, seg_loc, w_query, w_key, w_value, w_out):
        chunk = x_loc.shape[0]
        q_cols = w_query.shape[1]
        n_blk = chunk // Q_BLK
        n_pc = chunk // O_ROWS
        return pl.pallas_call(
            layer_kernel,
            name='layer',
            out_shape=pltpu.VMEM((chunk, w_out.shape[1]), BF16),
            in_specs=[any_spec] * 6,
            out_specs=pl.BlockSpec(memory_space=pltpu.VMEM),
            scratch_shapes=[
                pltpu.VMEM((4,) + w_out.shape, BF16),
                pltpu.VMEM((4, chunk, q_cols), BF16),
                pltpu.VMEM((2, 4 * chunk, 2 * HEAD_DIM), BF16),
                pltpu.VMEM((1, 4 * chunk), jnp.int32),
                dma((n_blk + 6,)), dma((2, 3)), dma((2, 3)), dma((3,)), dma((3,)), dma((6,)), dma((6,)), dma((5,)), dma((4,)),
                dma((4,)), dma((4, 7)), dma((4,)), dma((4, n_pc)),
            ],
            compiler_params=pltpu.CompilerParams(collective_id=0, has_side_effects=True, vmem_limit_bytes=59600000),
        )(x_loc, seg_loc[None, :], w_query, w_key, w_value, w_out)

    return jax.shard_map(layer, mesh=mesh, in_specs=(P(('dp', 'cp'), None), P(('dp', 'cp')), P(None, 'tp'), P(None, 'tp'), P(None, 'tp'), P('tp', None)), out_specs=P(('dp', 'cp'), None), check_vma=False)
```

```python
import functools

import jax
import jax.numpy as jnp
from jax import lax
from jax.experimental import pallas as pl
from jax.experimental.pallas import tpu as pltpu
from jax.sharding import PartitionSpec as P

HEAD_DIM = 128
MESH = pl.DeviceIdType.MESH
LOG2_SCALE = (HEAD_DIM ** -0.5) * 1.4426950408889634
F32 = jnp.float32
BF16 = jnp.bfloat16

Q_BLK = 256
LOC_BLK = 512
O_ROWS = 128


def coords():
    return lax.axis_index('dp'), lax.axis_index('tp'), lax.axis_index('cp')


def greet(dp, tp, cp, mid):
    bar = pltpu.get_barrier_semaphore()

    def hello(dev):
        pl.semaphore_signal(bar, inc=1, device_id=dev, device_id_type=MESH)

    hello((1 - dp, tp, cp))
    hello((dp, tp, lax.rem(cp + 2, 4)))
    hello((dp, tp, cp + 1 - 2 * lax.rem(cp, 2)))
    pl.when(tp > 0)(lambda: hello((dp, tp - 1, cp)))
    pl.when(tp < 3)(lambda: hello((dp, tp + 1, cp)))
    pl.semaphore_wait(bar, 4 + mid)


def peer_shard(tp, k):
    if k == 1:
        return tp + 1 - 2 * lax.rem(tp, 2)
    if k == 2:
        return 2 - tp // 2
    return 3 * (1 - tp // 2)


def layer_kernel(x_hbm, seg_hbm, wq_hbm, wk_hbm, wv_hbm, wo_hbm, y_ref,
                 w_v, o_v, kv_v, seg_v,
                 load_sem, kv_send, kv_recv, seg_send, seg_recv, x_send, x_recv, z_send, z_recv, w_send, w_recv, o_send, o_recv):
    dp, tp, cp = coords()
    mid = lax.rem((tp + 1) // 2, 2)
    core = lax.rem(cp, 2)
    chunk, d_model = x_hbm.shape
    q_cols = wq_hbm.shape[1]
    heads = q_cols // HEAD_DIM
    n_rows = wo_hbm.shape[0] // 8
    n_cols = wo_hbm.shape[1]
    part_a = n_cols // HEAD_DIM * 3 // 7 * HEAD_DIM
    x_rows = d_model // 8
    wx_cols = q_cols + 2 * HEAD_DIM
    n_blk = chunk // Q_BLK
    n_pc = chunk // O_ROWS
    per_blk = Q_BLK // O_ROWS
    cp_y = lax.rem(cp + 2, 4)
    cp_c = cp + 1 - 2 * core
    dev_x, dev_y, dev_c = (1 - dp, tp, cp), (dp, tp, cp_y), (dp, tp, cp_c)

    def onward(shard):
        return tp + 1 - 2 * (shard // (tp + 1) > 0).astype(jnp.int32)

    def rows_of(dp_i, cp_i):
        return pl.ds(pl.multiple_of((dp_i * 4 + cp_i) * n_rows, 16), n_rows)

    def z_copy(slot, src, shard, to):
        return pltpu.make_async_remote_copy(src, w_v.at[shard, rows_of(dp, cp)], z_send.at[slot], z_recv.at[shard],
                                            device_id=(dp, to, cp), device_id_type=MESH)

    z_up = z_copy(0, wo_hbm.at[rows_of(dp, cp)], tp, tp + 1)
    z_down = z_copy(4, wo_hbm.at[rows_of(dp, cp)], tp, tp - 1)

    def z_next(k):
        shard = peer_shard(tp, k)
        return z_copy(k, w_v.at[shard, rows_of(dp, cp)], shard, onward(shard))

    def x_slice(dp_i, cp_i, part='ab'):
        rows_a = x_rows * 3 // 7
        first = (dp_i * 4 + cp_i) * x_rows + (rows_a if part == 'b' else 0)
        return pl.ds(pl.multiple_of(first, 16), {'a': rows_a, 'b': x_rows - rows_a, 'ab': x_rows}[part])

    def wx_copies(wx_v, part):
        rows = x_slice(dp, cp, part)
        first = 3 * (part == 'b')
        out = []
        for n, (src, lo, hi) in enumerate(((wq_hbm, 0, q_cols), (wk_hbm, q_cols, q_cols + HEAD_DIM), (wv_hbm, q_cols + HEAD_DIM, wx_cols))):
            out.append(pltpu.make_async_remote_copy(src.at[rows], wx_v.at[rows, lo:hi], x_send.at[first + n], x_recv.at[first + n],
                                                    device_id=(dp, tp - 1 + 2 * (tp // 2), cp), device_id_type=MESH))
        return out

    cuts = {'a': pl.ds(0, part_a), 'b': pl.ds(part_a, n_cols - part_a), 'ab': pl.ds(0, n_cols)}
    hops = [('x', 'own', 'a'), ('x', 'own', 'b'), ('x', 'y', 'b'), ('y', 'own', 'b'), ('y', 'own', 'a'), ('y', 'x', 'a'),
            ('c', 'own', 'ab'), ('c', 'x', 'a'), ('c', 'x', 'b'), ('c', 'd', 'b'), ('c', 'y', 'b'), ('c', 'y', 'a'), ('c', 'd', 'a')]

    def holder(name, dp_i, cp_i):
        far = lax.rem(cp_i + 2, 4)
        return {'own': (dp_i, cp_i), 'x': (1 - dp_i, cp_i), 'y': (dp_i, far), 'd': (1 - dp_i, far)}[name]

    wx = []

    def w_hop(k, hop, dp_i, cp_i):
        route, name, part = hops[hop]
        if k == 4:
            at = wx[0].at[x_slice(*holder(name, dp_i, cp_i), part)]
        else:
            at = w_v.at[peer_shard(tp, k), rows_of(*holder(name, dp_i, cp_i)), cuts[part]]
        dev = {'x': dev_x, 'y': dev_y, 'c': dev_c}[route]
        return pltpu.make_async_remote_copy(at, at, w_send.at[k - 1], w_recv.at[k - 1, min(hop, 6)], device_id=dev, device_id_type=MESH)

    def w_copy(k, hop):
        return w_hop(k, hop, dp, cp)

    def w_arrival(k, hop):
        dp_i, cp_i = {'x': (1 - dp, cp), 'y': (dp, cp_y), 'c': (dp, cp_c)}[hops[hop][0]]
        return w_hop(k, hop, dp_i, cp_i)

    def w_arrived(k):
        z_next(k).wait_recv()
        pl.when(mid == 1)(lambda: z_next(k).start())

    def w_send_on(k, *which):
        for hop in which:
            w_copy(k, hop).start()

    def w_enter(k):
        w_arrived(k)
        w_send_on(k, 0, 3, 6, 1, 4)

    def w_relay(k, *which):
        after = {0: (5, 7), 1: (8,), 2: (9,), 3: (2, 10), 4: (11,), 5: (12,)}
        for hop in which:
            w_arrival(k, hop).wait_recv()
            w_send_on(k, *after[hop])

    def w_bulk(k, slices):
        at = wx[0].at[0:slices * x_rows] if k == 4 else w_v.at[peer_shard(tp, k), 0:slices * n_rows]
        return pltpu.make_async_remote_copy(at, at, w_send.at[k - 1], w_recv.at[k - 1, 6], device_id=dev_c, device_id_type=MESH)

    def w_finish(k):
        w_bulk(k, 4).wait_recv()

    def piece(c):
        return pl.ds(pl.multiple_of(c * O_ROWS, O_ROWS), O_ROWS)

    def each(first, what):
        @pl.loop(first, n_pc - per_blk)
        def _(n):
            what(nth(n))

        for c in range(per_blk):
            what(c)

    def nth(n):
        return (n_blk - 1 - n // per_blk) * per_blk + lax.rem(n, per_blk)

    o_cut = q_cols - 2 * HEAD_DIM

    def o_copy(slot, c, shard, to):
        if isinstance(c, int):
            at = o_v.at[shard, 0:Q_BLK, slice(0, o_cut) if c == 0 else slice(o_cut, q_cols)]
        else:
            at = o_v.at[shard, piece(c)]
        return pltpu.make_async_remote_copy(at, at, o_send.at[slot], o_recv.at[shard, c], device_id=(dp, to, cp), device_id_type=MESH)

    def o_own(c):
        return o_copy(0, c, tp, tp + 1 - 2 * (tp // 2))

    def o_leave(i):
        for j in range(per_blk):
            o_own(j if isinstance(i, int) else i * per_blk + j).start()

    def o_next(k, c):
        shard = peer_shard(tp, k)
        return o_copy(k, c, shard, onward(shard))

    def o_forward(k, c):
        o_next(k, c).wait_recv()
        pl.when(mid == 1)(lambda: o_next(k, c).start())

    def kv_copies(g, slot, block, to):
        rows = pl.ds(pl.multiple_of(block * chunk, chunk), chunk)
        dev = (dp, tp, to)
        kv = pltpu.make_async_remote_copy(kv_v.at[g, rows], kv_v.at[g, rows], kv_send.at[g, slot], kv_recv.at[g, slot],
                                          device_id=dev, device_id_type=MESH)
        if g == 1:
            return (kv,)
        return (kv, pltpu.make_async_remote_copy(seg_v.at[:, rows], seg_v.at[:, rows], seg_send.at[slot], seg_recv.at[slot],
            device_id=dev, device_id_type=MESH))

    def kv_leave(g):
        pl.when(cp < 2)(lambda: over(kv_copies(g, 0, cp, cp_y), 'start'))
        pl.when(core == 0)(lambda: over(kv_copies(g, 1, cp, cp_c), 'start'))

    def kv_wait(g):
        @pl.when(cp >= 2)
        def _():
            over(kv_copies(g, 0, cp - 2, cp), 'wait_recv')
            over(kv_copies(g, 2, cp - 2, cp_c), 'start')
            over(kv_copies(g, 2, cp_c - 2, cp), 'wait_recv')

        @pl.when(core == 1)
        def _():
            over(kv_copies(g, 1, cp_c, cp), 'wait_recv')

    def kv_sent(g):
        pl.when(cp < 2)(lambda: over(kv_copies(g, 0, cp, cp_y), 'wait_send'))
        pl.when(core == 0)(lambda: over(kv_copies(g, 1, cp, cp_c), 'wait_send'))
        pl.when(cp >= 2)(lambda: over(kv_copies(g, 2, cp - 2, cp_c), 'wait_send'))

    def over(copies, what):
        for copy in copies:
            getattr(copy, what)()

    own_w = pltpu.make_async_copy(wo_hbm, w_v.at[tp], load_sem.at[n_blk + 5])

    def attend(wx_v, w_blk, q_v, col_v, bias_v, m_v, l_v, acc_v):
        wx.append(wx_v)
        x_v = y_ref
        n_w = 2 * HEAD_DIM
        own = pl.ds(pl.multiple_of(cp * chunk, chunk), chunk)
        x_loads = []
        for i in range(n_blk):
            rows = slice(i * Q_BLK, (i + 1) * Q_BLK)
            x_loads.append(pltpu.make_async_copy(x_hbm.at[rows], x_v.at[rows], load_sem.at[i]))
        seg_load = pltpu.make_async_copy(seg_hbm, seg_v.at[:, own], load_sem.at[n_blk])
        spans = [(lo, min(lo + n_w, q_cols)) for lo in range(0, q_cols, n_w)]
        w_loads = [[pltpu.make_async_copy(wk_hbm, w_blk.at[0, :, 0:HEAD_DIM], load_sem.at[n_blk + 1]),
                    pltpu.make_async_copy(wv_hbm, w_blk.at[0, :, HEAD_DIM:n_w], load_sem.at[n_blk + 2])]]
        for n, (lo, hi) in enumerate(spans):
            w_loads.append([pltpu.make_async_copy(wq_hbm.at[:, lo:hi], w_blk.at[(n + 1) % 2, :, 0:hi - lo],
                                                  load_sem.at[n_blk + 3 + (n + 1) % 2])])
        over(w_loads[0], 'start')
        over(x_loads, 'start')
        over(w_loads[1], 'start')
        seg_load.start()

        greet(dp, tp, cp, mid)

        @pl.when(mid == 1)
        def _():
            over(wx_copies(wx_v, 'a'), 'start')
            over(wx_copies(wx_v, 'b'), 'start')

        pl.when(tp < 3)(z_up.start)
        pl.when(tp > 0)(z_down.start)

        def blk(i):
            return pl.ds(pl.multiple_of(i * Q_BLK, Q_BLK), Q_BLK)

        def own_rows(i):
            return pl.ds(pl.multiple_of(cp * chunk + i * Q_BLK, Q_BLK), Q_BLK)

        def product(i, w):
            return jnp.dot(x_v[blk(i), :], w, preferred_element_type=F32).astype(BF16)

        over(w_loads[0], 'wait')

        @pl.loop(0, n_blk)
        def _(i):
            pltpu.make_async_copy(x_hbm.at[blk(i)], x_v.at[blk(i)], load_sem.at[i]).wait()
            kv_v[0, own_rows(i), :] = product(i, w_blk[0])

        over(w_loads[2], 'start')
        seg_load.wait()
        for n, (lo, hi) in enumerate(spans):
            over(w_loads[n + 1], 'wait')

            @pl.loop(0, n_blk)
            def _(i):
                q_v[blk(i), lo:hi] = product(i, w_blk[(n + 1) % 2, :, 0:hi - lo])
                if n == 0:
                    pl.when(i == 0)(lambda: kv_leave(0))

            if n + 3 < len(w_loads):
                over(w_loads[n + 3], 'start')
        own_w.start()

        @pl.loop(0, chunk // HEAD_DIM)
        def _(i):
            ids = seg_v[0:1, pl.ds(pl.multiple_of(cp * chunk + i * HEAD_DIM, HEAD_DIM), HEAD_DIM)]
            rows = pl.ds(pl.multiple_of(i * HEAD_DIM, HEAD_DIM), HEAD_DIM)
            col_v[rows, :] = jnp.transpose(jnp.broadcast_to(ids, (HEAD_DIM, HEAD_DIM)))

        @pl.when(mid == 0)
        def _():
            over(wx_copies(wx_v, 'a'), 'wait_recv')
            w_send_on(4, 0, 4)

        def step(g, i, key0, n_keys, first):
            keys = pl.ds(pl.multiple_of(key0, n_keys), n_keys)
            groups = n_keys // HEAD_DIM
            q_seg = col_v[blk(i), :]
            for n in range(groups):
                cols = pl.ds(pl.multiple_of(key0 + n * HEAD_DIM, HEAD_DIM), HEAD_DIM)
                ok = q_seg == seg_v[0:1, cols]
                if first:
                    q_pos = cp * chunk + i * Q_BLK + lax.broadcasted_iota(jnp.int32, (Q_BLK, HEAD_DIM), 0)
                    k_pos = key0 + n * HEAD_DIM + lax.broadcasted_iota(jnp.int32, (Q_BLK, HEAD_DIM), 1)
                    ok = ok & (q_pos >= k_pos)
                bias_v[:, n * HEAD_DIM:(n + 1) * HEAD_DIM] = jnp.where(ok, 0.0, -jnp.inf)
            k_blk = kv_v[g, keys, 0:HEAD_DIM]
            v_blk = kv_v[g, keys, HEAD_DIM:2 * HEAD_DIM]

            def scores(h):
                return lax.dot_general(q_v[blk(i), h * HEAD_DIM:(h + 1) * HEAD_DIM], k_blk, (((1,), (1,)), ((), ())),
                                       preferred_element_type=F32)

            ahead = scores(0)
            for h in range(heads):
                cols = slice(h * HEAD_DIM, (h + 1) * HEAD_DIM)
                s = ahead
                if h + 1 < heads:
                    ahead = scores(h + 1)
                s = [s[:, n * HEAD_DIM:(n + 1) * HEAD_DIM] + bias_v[:, n * HEAD_DIM:(n + 1) * HEAD_DIM] for n in range(groups)]
                top = jnp.max(functools.reduce(jnp.maximum, s), axis=1, keepdims=True)
                if first:
                    m_new = jnp.broadcast_to(top, (Q_BLK, HEAD_DIM))
                else:
                    m_old = m_v[:, cols]
                    m_new = jnp.maximum(m_old, top)
                    fade = jnp.exp2((m_old - m_new) * LOG2_SCALE)
                p = [jnp.exp2((part - m_new) * LOG2_SCALE) for part in s]
                total = functools.reduce(jnp.add, p)
                probs = jnp.concatenate([part.astype(BF16) for part in p], axis=1)
                pv = jnp.dot(probs, v_blk, preferred_element_type=F32)
                m_v[:, cols] = m_new
                if first:
                    l_v[:, cols] = total
                    acc_v[:, cols] = pv
                else:
                    l_v[:, cols] = l_v[:, cols] * fade + total
                    acc_v[:, cols] = acc_v[:, cols] * fade + pv

        per_loc = LOC_BLK // Q_BLK

        def attention(g, shard, after_first, inside, after_block):
            @pl.loop(0, n_blk)
            def _(t):
                i = n_blk - 1 - t
                last = i // per_loc
                odd = lax.rem(i, per_loc)
                pl.when(odd == 1)(lambda: step(g, i, cp * chunk + last * LOC_BLK, LOC_BLK, True))
                pl.when(odd == 0)(lambda: step(g, i, cp * chunk + i * Q_BLK, Q_BLK, True))
                after_first(t)

                @pl.loop(0, last)
                def _(j):
                    step(g, i, cp * chunk + j * LOC_BLK, LOC_BLK, False)

                pl.when(t == 0)(lambda: kv_wait(g))

                @pl.loop(0, cp)
                def _(j):
                    step(g, i, j * chunk, chunk, False)
                    if inside is not None:
                        pl.when((t == 0) & (j == 0))(inside)

                if inside is not None:
                    pl.when((t == 0) & (cp == 0))(inside)
                for h in range(heads):
                    cols = slice(h * HEAD_DIM, (h + 1) * HEAD_DIM)
                    total = jnp.sum(l_v[:, cols], axis=1, keepdims=True)
                    o_v[shard, blk(i), cols] = (acc_v[:, cols] / total).astype(BF16)
                after_block(t)

        def own_after_first(t):
            pl.when(t > 0)(lambda: o_leave(n_blk - t))
            pl.when((t == 3) & (mid == 0))(lambda: w_relay(4, 2, 5))

        def own_inside():
            @pl.when(mid == 1)
            def _():
                w_enter(1)
                w_enter(2)

            @pl.when(mid == 0)
            def _():
                over(wx_copies(wx_v, 'b'), 'wait_recv')
                w_send_on(4, 3, 1, 6)

        def own_after_block(t):
            pl.when((t == 1) & (mid == 1))(lambda: w_enter(3))
            pl.when((t == 0) & (mid == 0))(lambda: w_relay(4, 0, 4))

            @pl.when((t == 1) & (mid == 0))
            def _():
                w_relay(4, 3, 1)
                w_arrived(1)
                w_send_on(1, 0, 3, 6, 1, 4)

        attention(0, tp, own_after_first, own_inside, own_after_block)

        @pl.when(mid == 0)
        def _():
            w_finish(4)

            @pl.loop(0, n_blk)
            def _(i):
                kv_v[1, own_rows(i), :] = product(i, wx_v[:, q_cols:wx_cols])

            o_leave(0)

            @pl.loop(0, n_blk)
            def _(i):
                q_v[blk(i), :] = product(i, wx_v[:, 0:q_cols])

                @pl.when(i == 0)
                def _():
                    kv_leave(1)
                    w_relay(1, 0, 3)
                    w_enter(2)

            def more_after_first(t):
                pl.when(t == 2)(lambda: w_relay(1, 2, 5))

            def more_after_block(t):
                @pl.when(t == 0)
                def _():
                    w_relay(1, 1, 4)
                    w_enter(3)

                pl.when(t == 1)(lambda: w_relay(2, 0, 3))
                pl.when(t == 2)(lambda: w_relay(2, 1, 4))

            attention(1, peer_shard(tp, 1), more_after_first, None, more_after_block)
            w_bulk(4, 7).wait_send()

        @pl.when(mid == 1)
        def _():
            over(wx_copies(wx_v, 'a'), 'wait_send')
            over(wx_copies(wx_v, 'b'), 'wait_send')

    pl.run_scoped(
        attend,
        pltpu.VMEM((d_model, wx_cols), BF16),
        pltpu.VMEM((2, d_model, 2 * HEAD_DIM), BF16),
        pltpu.VMEM((chunk, q_cols), BF16),
        pltpu.VMEM((chunk, HEAD_DIM), jnp.int32),
        pltpu.VMEM((Q_BLK, chunk), F32),
        pltpu.VMEM((Q_BLK, q_cols), F32),
        pltpu.VMEM((Q_BLK, q_cols), F32),
        pltpu.VMEM((Q_BLK, q_cols), F32),
    )

    def output(acc_v):
        n_tile = 256

        def multiply(ks, rows, width, store, between):
            @pl.loop(0, n_cols // width)
            def _(n):
                out = pl.ds(pl.multiple_of(n * width, width), width)
                parts = []
                for k in ks:
                    shard = tp if k == 0 else peer_shard(tp, k)
                    parts.append(jnp.dot(o_v[shard, rows, :], w_v[shard, :, out], preferred_element_type=F32))
                store(out, functools.reduce(jnp.add, parts))
                if between is not None:
                    between(n)

        own_w.wait()

        @pl.when(mid == 1)
        def _():
            w_relay(1, 0, 3)
            o_leave(0)
            w_relay(2, 0, 3)
            w_relay(1, 1, 4)
            w_relay(2, 1, 4)

            def both(c):
                o_forward(1, c)
                o_forward(2, c)

            each(0, both)

            w_relay(3, 0, 3, 1, 4)
            w_relay(1, 2, 5)

        pl.when(mid == 0)(lambda: w_relay(3, 0))
        w_finish(1)

        def during_first(n):
            pl.when((n == 4) & (mid == 0))(lambda: w_relay(3, 3))

            @pl.when(n == 8)
            def _():
                w_relay(2, 2, 5)
                pl.when(mid == 0)(lambda: w_relay(3, 1))

            pl.when((n == 11) & (mid == 0))(lambda: w_relay(3, 4))

        def during_second(n):
            pl.when(n == 9)(lambda: w_relay(3, 2, 5))

        def begin(out, part):
            acc_v[:, out] = part

        def add(out, part):
            acc_v[:, out] += part

        multiply((0, 1), slice(None), n_tile, begin, during_first)
        w_finish(2)

        pl.when(mid == 0)(lambda: each(0, lambda c: o_next(2, c).wait_recv()))

        @pl.when(mid == 1)
        def _():
            @pl.loop(0, n_pc // 2)
            def _(n):
                o_forward(3, nth(n))

        multiply((2,), slice(None), n_tile, add, during_second)
        w_finish(3)

        pl.when(mid == 1)(lambda: each(n_pc // 2, lambda c: o_forward(3, c)))

        def last_shard(rows, pieces, cols, width, store):
            @pl.when(mid == 0)
            def _():
                for c in pieces:
                    o_next(3, c).wait_recv()

            shard = peer_shard(tp, 3)

            @pl.loop(0, n_cols // width)
            def _(n):
                out = pl.ds(pl.multiple_of(n * width, HEAD_DIM), width)
                store(rows, out, jnp.dot(o_v[shard, rows, cols], w_v[shard, cols, out], preferred_element_type=F32))

        def settle(rows, out, part):
            y_ref[rows, out] = (acc_v[rows, out] + part).astype(BF16)

        def gather(rows, out, part):
            acc_v[rows, out] += part

        def leaving(lo, hi):
            return [jnp.int32((n_blk - 1 - n // per_blk) * per_blk + n % per_blk) for n in range(lo, hi)]

        last_shard(slice(chunk // 2, chunk), leaving(0, n_pc // 2), slice(0, q_cols), 2 * n_tile, settle)
        last_shard(slice(Q_BLK, chunk // 2), leaving(n_pc // 2, n_pc - per_blk), slice(0, q_cols), 2 * n_tile, settle)
        last_shard(slice(0, Q_BLK), [0], slice(0, o_cut), n_cols // 4, gather)
        last_shard(slice(0, Q_BLK), [1], slice(o_cut, q_cols), n_cols // 2, settle)

    pl.run_scoped(output, pltpu.VMEM((chunk, n_cols), F32))

    kv_sent(0)

    pl.when(mid == 0)(lambda: kv_sent(1))
    pl.when(tp < 3)(z_up.wait_send)
    pl.when(tp > 0)(z_down.wait_send)
    for k in (1, 2, 3):
        pl.when(mid == 1)(lambda: z_next(k).wait_send())
        w_bulk(k, 7).wait_send()

    def o_sent(slot, shard):
        at = o_v.at[shard]
        pltpu.make_async_remote_copy(at, at, o_send.at[slot], o_recv.at[shard, 0], device_id=dev_c, device_id_type=MESH).wait_send()

    o_sent(0, tp)

    @pl.when(mid == 1)
    def _():
        for k in (1, 2, 3):
            o_sent(k, peer_shard(tp, k))


def solution(mesh):
    any_spec = pl.BlockSpec(memory_space=pl.ANY)
    dma = pltpu.SemaphoreType.DMA

    def layer(x_loc, seg_loc, w_query, w_key, w_value, w_out):
        chunk = x_loc.shape[0]
        q_cols = w_query.shape[1]
        n_blk = chunk // Q_BLK
        n_pc = chunk // O_ROWS
        return pl.pallas_call(
            layer_kernel,
            name='layer',
            out_shape=pltpu.VMEM((chunk, w_out.shape[1]), BF16),
            in_specs=[any_spec] * 6,
            out_specs=pl.BlockSpec(memory_space=pltpu.VMEM),
            scratch_shapes=[
                pltpu.VMEM((4,) + w_out.shape, BF16),
                pltpu.VMEM((4, chunk, q_cols), BF16),
                pltpu.VMEM((2, 4 * chunk, 2 * HEAD_DIM), BF16),
                pltpu.VMEM((1, 4 * chunk), jnp.int32),
                dma((n_blk + 6,)), dma((2, 3)), dma((2, 3)), dma((3,)), dma((3,)), dma((6,)), dma((6,)), dma((5,)), dma((4,)),
                dma((4,)), dma((4, 7)), dma((4,)), dma((4, n_pc)),
            ],
            compiler_params=pltpu.CompilerParams(collective_id=0, has_side_effects=True, vmem_limit_bytes=59600000),
        )(x_loc, seg_loc[None, :], w_query, w_key, w_value, w_out)

    return jax.shard_map(layer, mesh=mesh, in_specs=(P(('dp', 'cp'), None), P(('dp', 'cp')), P(None, 'tp'), P(None, 'tp'), P(None, 'tp'), P('tp', None)), out_specs=P(('dp', 'cp'), None), check_vma=False)
```
